32 devices in a mesh: gx: 4 (over x, core), gy: 8 (over z, y).
Axes of the slice: x: 2, y: 2, z: 4, core: 2. Of those that a mesh axis runs over, the one named last changes fastest.
Arguments:
- concentration: float32 [192, 5, 32768], P(('gx', 'gy')), may hold values from 0.05 to 3
- neighbours: int32 [192, 6], P(('gx', 'gy')), may hold values from -1 to 191, as said below
- source_slot: int32 [192], P(('gx', 'gy')), may hold values from -1 to 191, as said below
- mobility: float32 [5], replicated, may hold values from 0.3 to 2
- fermi_gain: float32 [5], replicated, may hold values from 0.3 to 3
- rates: float32 [5], replicated, may hold values from 0.05 to 0.5
Outputs:
- moved: float32 [192, 5, 32768], P(('gx', 'gy'))
The draws below stay inside these ranges and needn't reach their ends.
Inputs may be any that keep to these rules, and one draw needn't show every extreme that they name: neighbours: each entry is -1 or a slot on the same device or on a device next to it along gx or along gy (same index on the other axis); every slot that source_slot names has neighbours that name only such slots that source_slot names too or -1. source_slot: each entry is -1 or a slot on the same device or on a device next to it along gx or along gy; no slot is named twice; only slots below 2 of a device are other than -1; at most 1 slots of one device name slots of one other device, and some device names exactly 1 of a neighbour's.
All inputs are finite; a program needn't handle non-finite values.
Results may differ from the reference program's by a relative error of at most 0.0003.
Values sent between devices are 32-bit elements; how exact they have to be, the bound alone decides.
No kernel may reach another device: no remote copies, remote signals or barrier semaphores. Data moves between devices by JAX's collectives and lax.ppermute only.
A program may use at most 192 MiB of HBM per device.

```python
import math
import jax
import jax.numpy as jnp
from jax import lax

B = 32
SPECIES = 5
SWEEPS = 3
KEEP = 2
MOVE = 1
CAP = 6
PATCHES = 192
CELLS = 32768
N_GX = 4
N_GY = 8


DIRECTIONS = ((-1, 0), (1, 0), (0, -1), (0, 1))


def plan_layout(key):
    layout_key = jax.random.fold_in(key, 4099)
    shift_key, light_key, order_key = jax.random.split(layout_key, 3)
    device_count = N_GX * N_GY
    device_ids = jnp.arange(device_count, dtype=jnp.int32)
    column_index = device_ids // N_GY
    row_index = device_ids % N_GY
    offset = jax.random.randint(shift_key, (), 0, 5)
    crowded = (column_index + 2 * row_index + offset) % 5 == 0
    present = jnp.stack([(column_index + step_x >= 0) & (column_index + step_x < N_GX) & (row_index + step_y >= 0) & (row_index + step_y < N_GY) for step_x, step_y in DIRECTIONS], axis=1)
    neighbour_ids = jnp.stack([jnp.clip(column_index + step_x, 0, N_GX - 1) * N_GY + jnp.clip(row_index + step_y, 0, N_GY - 1) for step_x, step_y in DIRECTIONS], axis=1).astype(jnp.int32)
    light_live = jax.random.randint(light_key, (device_count,), 1, KEEP)
    live = jnp.where(crowded, KEEP + MOVE * jnp.sum(present.astype(jnp.int32), axis=1), light_live).astype(jnp.int32)

    def shuffle(device_key):
        return jax.random.permutation(device_key, CAP)
    home = jax.vmap(shuffle)(jax.random.split(order_key, device_count)).astype(jnp.int32)
    return (device_ids, crowded, present, neighbour_ids, live, home)


def draw_source_slot(key, part):
    device_ids, crowded, present, neighbour_ids, live, home = plan_layout(key)
    slots = jnp.arange(CAP, dtype=jnp.int32)
    kept = jnp.where(crowded, KEEP, live)
    result = jnp.where(slots[None, :] < kept[:, None], device_ids[:, None] * CAP + home, -1)
    for direction in range(4):
        helper_device = neighbour_ids[:, direction]
        receives = present[:, direction] & crowded[helper_device] & jnp.logical_not(crowded)
        backward = direction ^ 1
        rank = jnp.sum(present[helper_device][:, :backward].astype(jnp.int32), axis=1)
        logical = KEEP + rank[:, None] * MOVE + (slots[None, :] - live[:, None])
        within = receives[:, None] & (slots[None, :] >= live[:, None]) & (slots[None, :] < live[:, None] + MOVE)
        position = jnp.take_along_axis(home[helper_device], jnp.clip(logical, 0, CAP - 1), axis=1)
        result = jnp.where(within, helper_device[:, None] * CAP + position, result)
    return result.reshape(-1).astype(jnp.int32)


def draw_neighbours(key, part):
    device_ids, crowded, present, neighbour_ids, live, home = plan_layout(key)
    device_count = N_GX * N_GY
    face_key = jax.random.fold_in(key, 8191)
    heading_key, slot_key = jax.random.split(face_key, 2)
    heading = jax.random.randint(heading_key, (device_count, CAP * 6), 0, 6)
    candidates = jnp.concatenate([device_ids[:, None], neighbour_ids], axis=1)
    exists = jnp.concatenate([jnp.ones((device_count, 1), dtype=bool), present], axis=1)
    clipped = jnp.minimum(heading, 4)
    target = jnp.take_along_axis(candidates, clipped, axis=1)
    valid = (heading < 5) & jnp.take_along_axis(exists, clipped, axis=1)
    raw = jax.random.randint(slot_key, (device_count, CAP * 6), 0, 1 << 20)
    logical = raw % live[target]
    position = home[target, logical]
    result = jnp.where(valid, target * CAP + position, -1)
    return result.reshape(device_count * CAP, 6).astype(jnp.int32)


def steps_of(rng, shape, cuts, smallest, high):
    gain, own = 1.0, jax.random.fold_in(rng, 6)
    for dim, shards_of in cuts:
        draws = jnp.exp(jax.random.uniform(jax.random.fold_in(own, dim), (shards_of,), jnp.float32, smallest / len(cuts), high / len(cuts)))
        gain = gain * jnp.repeat(draws, shape[dim] // shards_of).reshape([-1 if axis == dim else 1 for axis in range(len(shape))])
    return gain


def setup_inputs(seed: int = 0) -> dict:
    key_of = jax.random.split(jax.random.key(seed), 7)
    return {
        "concentration": jnp.clip(jnp.exp(math.log(3.0) - 4.0943445 * jax.random.uniform(key_of[0], (PATCHES, SPECIES, CELLS), jnp.float32) ** steps_of(key_of[0], (PATCHES, SPECIES, CELLS), ((0, 32),), -0.2, 0.2)), 0.05, 3.0),
        "neighbours": draw_neighbours(jax.random.fold_in(key_of[6], 71), 0),
        "source_slot": draw_source_slot(jax.random.fold_in(key_of[6], 71), 0),
        "mobility": jnp.clip(jnp.exp(jax.random.uniform(key_of[3], (SPECIES,), jnp.float32, math.log(0.3), math.log(2.0))), 0.3, 2.0),
        "fermi_gain": jnp.clip(jnp.exp(jax.random.uniform(key_of[4], (SPECIES,), jnp.float32, math.log(0.3), math.log(3.0))), 0.3, 3.0),
        "rates": jnp.clip(jnp.exp(jax.random.uniform(key_of[5], (5,), jnp.float32, math.log(0.05), math.log(0.5))), 0.05, 0.5),
    }


OPPOSITE = (1, 0, 3, 2, 5, 4)

def faces_of(blocks):
    last = blocks.shape[-1] - 1
    return jnp.stack([blocks[..., 0, :, :], blocks[..., last, :, :], blocks[..., :, 0, :], blocks[..., :, last, :], blocks[..., :, :, 0], blocks[..., :, :, last]], axis=-4)

def neighbour_sum(iterate, ghosts):
    lower_x = jnp.concatenate([ghosts[0][:, None], iterate[:, :-1]], axis=1)
    upper_x = jnp.concatenate([iterate[:, 1:], ghosts[1][:, None]], axis=1)
    lower_y = jnp.concatenate([ghosts[2][:, :, None], iterate[:, :, :-1]], axis=2)
    upper_y = jnp.concatenate([iterate[:, :, 1:], ghosts[3][:, :, None]], axis=2)
    lower_z = jnp.concatenate([ghosts[4][..., None], iterate[..., :-1]], axis=3)
    upper_z = jnp.concatenate([iterate[..., 1:], ghosts[5][..., None]], axis=3)
    return lower_x + upper_x + lower_y + upper_y + lower_z + upper_z

def smooth(current, ghosts, mobility, fermi_gain, rates):
    dopant_sum = current[0] + current[3] + current[4]
    half_total = 0.5 * dopant_sum
    electrons = half_total + jnp.sqrt(half_total * half_total + 1.0)
    gain_column = fermi_gain[:, None, None, None]
    spread = mobility[:, None, None, None] * (1.0 + gain_column * electrons[None]) / (1.0 + gain_column)
    dopant, interstitial, vacancy, pair_inter, pair_vacancy = (current[0], current[1], current[2], current[3], current[4])
    forming_ai = rates[0] * dopant * interstitial - rates[1] * pair_inter
    forming_av = rates[2] * dopant * vacancy - rates[3] * pair_vacancy
    recombine = rates[4] * (interstitial * vacancy - 1.0)
    source = jnp.stack([dopant - forming_ai - forming_av, interstitial - forming_ai - recombine, vacancy - forming_av - recombine, pair_inter + forming_ai, pair_vacancy + forming_av], axis=0)
    diagonal = 1.0 + 6.0 * spread
    iterate = current
    for repeat in range(SWEEPS):
        iterate = (source + spread * neighbour_sum(iterate, ghosts)) / diagonal
    return iterate

def reference(concentration, neighbours, source_slot, mobility, fermi_gain, rates):
    patches = concentration.shape[0]
    blocks = concentration.reshape(patches, SPECIES, B, B, B)
    face_table = faces_of(blocks)
    opposite = jnp.array(OPPOSITE, jnp.int32)
    face_ids = jnp.arange(6, dtype=jnp.int32)

    def one_slot(source):
        patch_index = jnp.maximum(source, 0)
        neighbour_row = neighbours[patch_index]
        remote = face_table[jnp.maximum(neighbour_row, 0), opposite]
        own_layers = face_table[patch_index, face_ids]
        ghosts = jnp.where((neighbour_row >= 0)[:, None, None, None], remote, own_layers)
        swept = smooth(blocks[patch_index], ghosts, mobility, fermi_gain, rates)
        swept = jnp.where(source >= 0, swept, jnp.zeros_like(swept))
        return swept.reshape(SPECIES, B * B * B)
    return lax.map(one_slot, source_slot)
```

```python
import functools

import jax
import jax.numpy as jnp
from jax import lax
from jax.experimental import pallas as pl
from jax.experimental.pallas import tpu as pltpu
from jax.sharding import PartitionSpec as P

B = 32
SPECIES = 5
SWEEPS = 3
KEEP = 2
MOVE = 1
WORKING = KEEP - 1 + MOVE
SIDES = 6
TILES = B * B // 128
LAYER = (TILES, 128)
PAD = 2 * TILES

VMEM = pl.BlockSpec(memory_space=pltpu.VMEM)
SMEM = pl.BlockSpec(memory_space=pltpu.SMEM)
ANY = pl.BlockSpec(memory_space=pl.ANY)
F32 = jnp.float32


def iotas():
    sub = lax.broadcasted_iota(jnp.int32, LAYER, 0)
    lane = lax.broadcasted_iota(jnp.int32, LAYER, 1)
    return sub, lane


def pack_kernel(cap, c_ref, dense_ref, faces_ref, raw, sems):
    def copy(s):
        return pltpu.make_async_copy(c_ref.at[s], raw.at[s, :, pl.ds(0, cap), :], sems.at[s])

    for s in range(SPECIES):
        copy(s).start()
    rows = raw.reshape(SPECIES * B * TILES * 8, 128)
    _, lane = iotas()
    z = lane & (B - 1)
    quarter = lane // B
    per_x = TILES * 8

    def species(s, carry):
        copy(s).wait()
        base = s * (B * per_x)

        def slot(p, carry2):
            start = base + p
            z_first = z_last = None
            for x in range(B):
                v = rows[pl.ds(start + x * per_x, TILES, stride=8), :]
                dense_ref[p, s, x] = v
                a = v if x == 0 else pltpu.roll(v, x, 1)
                b = v if x == B - 1 else pltpu.roll(v, 128 + x - (B - 1), 1)
                z_first = a if x == 0 else jnp.where(z == x, a, z_first)
                z_last = b if x == 0 else jnp.where(z == x, b, z_last)
                if x == 0:
                    faces_ref[p * SIDES + 0, s] = v
                if x == B - 1:
                    faces_ref[p * SIDES + 1, s] = v
            y_first = y_last = None
            for j in range(4):
                a = rows[pl.ds(start + j * per_x, TILES, stride=4 * per_x), :]
                b = rows[pl.ds(start + j * per_x + (TILES - 1) * 8, TILES, stride=4 * per_x), :]
                a = a if j == 0 else pltpu.roll(a, j * B, 1)
                b = b if j == 3 else pltpu.roll(b, (j + 1) * B, 1)
                y_first = a if j == 0 else jnp.where(quarter == j, a, y_first)
                y_last = b if j == 0 else jnp.where(quarter == j, b, y_last)
            faces_ref[p * SIDES + 2, s] = y_first
            faces_ref[p * SIDES + 3, s] = y_last
            faces_ref[p * SIDES + 4, s] = z_first
            faces_ref[p * SIDES + 5, s] = z_last
            return carry2

        return lax.fori_loop(0, cap, slot, carry)

    lax.fori_loop(0, SPECIES, species, 0)


class Meta:
    def __init__(self, cap):
        self.cap = cap
        self.take_dev = 0
        self.take_loc = cap
        self.side_dev = 2 * cap
        self.side_loc = 2 * cap + SIDES * cap
        self.me = 2 * cap + 2 * SIDES * cap
        self.width = self.me + 4

    def build(self, neighbours, source_slot, me):
        def split(v):
            return jnp.where(v >= 0, v // self.cap, -1), jnp.maximum(v, 0) % self.cap

        parts = (*split(source_slot), *split(neighbours.reshape(-1)), jnp.full((4,), me))
        return jnp.concatenate([part.astype(jnp.int32) for part in parts])


def wanted(meta, take, slot, side, tables):
    ref, base = take
    dev = ref[base + meta.take_dev + slot]
    loc = ref[base + meta.take_loc + slot]
    cell = loc * SIDES + side
    near_dev = jnp.int32(-1)
    near_loc = jnp.int32(0)
    known = jnp.bool_(False)
    for table_dev, table, offset in tables:
        hit = dev == table_dev
        known = known | hit
        near_dev = jnp.where(hit, table[offset + meta.side_dev + cell], near_dev)
        near_loc = jnp.where(hit, table[offset + meta.side_loc + cell], near_loc)
    inner = near_dev < 0
    q_dev = jnp.where(known, jnp.where(inner, dev, near_dev), -1)
    q_loc = jnp.where(inner, loc, near_loc)
    face = jnp.where(inner, side, side ^ 1)
    return dev, q_dev, q_loc * SIDES + face


def copy_face(dst, dst_at, src, src_at):
    for s in range(SPECIES):
        dst[dst_at, s] = src[src_at, s]


def patches_kernel(meta, rows, own, xm, xp, ym, yp, dense_ref, to_xp, to_xm, to_yp, to_ym):
    me = own[meta.me]

    def send(table, out):
        pick = jnp.int32(0)
        for t in range(WORKING):
            hit = table[meta.take_dev + t] == me
            pick = jnp.where(hit, table[meta.take_loc + t], pick)

        def layer(x, carry):
            for s in range(SPECIES):
                out[s, x] = dense_ref[pick, s, x]
            return carry

        lax.fori_loop(0, B, layer, 0, unroll=4)

    send(yp, to_yp)
    send(ym, to_ym)
    send(xp, to_xp)
    send(xm, to_xm)


def faces_kernel(
    meta, rows, own, xm, xp, ym, yp, y2m, y2p, f_own, f_xm, f_xp,
    to_yp, to_ym, to_xp, to_xm, to_y2p, to_y2m, ghosts, plan,
):
    me = own[meta.me]
    width = meta.width

    def row_of_faces(dst, at, q_dev, q_face):
        for dev, src in ((me, f_own), (me - rows, f_xm), (me + rows, f_xp)):
            pl.when(q_dev == dev)(functools.partial(copy_face, dst, at, src, q_face))

    for step, table, out in ((1, yp, to_yp), (-1, ym, to_ym)):
        there = me + step
        tables = (
            (there, table, 0),
            (there - rows, table, width),
            (there + rows, table, 2 * width),
            (me, own, 0),
        )
        for t in range(WORKING):

            def side_of(f, carry, t=t, table=table, tables=tables, out=out):
                _, q_dev, q_face = wanted(meta, (table, 0), t, f, tables)
                row_of_faces(out, t * SIDES + f, q_dev, q_face)
                return carry

            lax.fori_loop(0, SIDES, side_of, 0)

    for step, table, out, far in ((1, xp, to_xp, f_xm), (-1, xm, to_xm, f_xp)):
        for t in range(WORKING):

            def side_of(f, carry, t=t, table=table, out=out, far=far, step=step):
                dev, q_dev, q_face = wanted(meta, (table, 0), t, f, ((me, own, 0),))
                hit = q_dev == me - step * rows
                pl.when(hit)(functools.partial(copy_face, out, f, far, q_face))
                return carry

            lax.fori_loop(0, SIDES, side_of, 0)

    for step, table, near, out in ((1, y2p, yp, to_y2p), (-1, y2m, ym, to_y2m)):
        for t in range(WORKING):

            def side_of(f, carry, t=t, table=table, near=near, out=out, step=step):
                dev, q_dev, q_face = wanted(meta, (table, 0), t, f, ((me + step, near, 0),))
                pl.when(q_dev == me)(functools.partial(copy_face, out, f, f_own, q_face))
                return carry

            lax.fori_loop(0, SIDES, side_of, 0)

    tables = (
        (me, own, 0),
        (me - rows, xm, 0),
        (me + rows, xp, 0),
        (me - 1, ym, 0),
        (me + 1, yp, 0),
    )
    for t in range(WORKING):
        dev = own[meta.take_dev + t]
        for c, table_dev in ((1, me - rows), (2, me + rows), (3, me - 1), (4, me + 1)):
            pl.when(dev == table_dev)(functools.partial(plan.__setitem__, 2 * WORKING * SIDES + t, c))
        pl.when(dev == me)(functools.partial(plan.__setitem__, 2 * WORKING * SIDES + t, 0))
        pl.when(dev < 0)(functools.partial(plan.__setitem__, 2 * WORKING * SIDES + t, -1))
        plan[2 * WORKING * SIDES + WORKING + t] = own[meta.take_loc + t]

        def side_of(f, carry, t=t):
            _, q_dev, q_face = wanted(meta, (own, 0), t, f, tables)
            at = t * SIDES + f
            row_of_faces(ghosts, at, q_dev, q_face)
            kind = jnp.int32(0)
            place = at
            for c, far in ((3, me - 2 * rows), (4, me + 2 * rows), (5, me - 2), (6, me + 2)):
                hit = q_dev == far
                kind = jnp.where(hit, c, kind)
                place = jnp.where(hit, f, place)
            row = me % rows
            q_row = q_dev % rows
            near = (q_dev == me - 1) | (q_dev == me - 1 - rows) | (q_dev == me - 1 + rows)
            kind = jnp.where((q_dev >= 0) & near & (q_row + 1 == row), 1, kind)
            near = (q_dev == me + 1) | (q_dev == me + 1 - rows) | (q_dev == me + 1 + rows)
            kind = jnp.where((q_dev >= 0) & near & (q_row == row + 1), 2, kind)
            plan[at] = kind
            plan[WORKING * SIDES + at] = place
            return carry

        lax.fori_loop(0, SIDES, side_of, 0)


def sweep_kernel(
    cap, plan, mob, gain, rates, dense_ref, p_xm, p_xp, p_ym, p_yp,
    ghosts, g_ym, g_yp, g_xm, g_xp, g_y2m, g_y2p,
    out_ref, ghost, grid, fixed, factor, stage, sems,
):
    sub, lane = iotas()
    z = lane & (B - 1)
    z_low, z_high = z == 0, z == B - 1
    y_low = (sub == 0) & (lane < B)
    y_high = (sub == TILES - 1) & (lane >= 128 - B)
    zero = jnp.zeros(LAYER, F32)

    stage_rows = stage.reshape(SPECIES * B * TILES * 8, 128)

    def clear(i, carry):
        stage_rows[pl.ds(pl.multiple_of(i * 8, 8), 8), :] = zero
        return carry

    lax.fori_loop(0, SPECIES * B * TILES, clear, 0, unroll=16)

    def clear_pad(i, carry):
        for a in range(2):
            for s in range(SPECIES):
                grid[a, s, pl.ds(pl.multiple_of(i * PAD, 8), TILES), :] = zero
        return carry

    lax.fori_loop(0, B + 1, clear_pad, 0)

    def full(value):
        return jnp.full(LAYER, value, F32)

    flat, slope = [], []
    for s in range(SPECIES):
        m, g = full(mob[s]), full(gain[s])
        flat.append(m / (1.0 + g))
        slope.append(m * g / (1.0 + g))
    rate = [full(rates[i]) for i in range(5)]

    for t in range(WORKING):
        kind_of_patch = plan[2 * WORKING * SIDES + t]
        place_of_patch = plan[2 * WORKING * SIDES + WORKING + t]

        def gather(f, carry, t=t):
            kind = plan[t * SIDES + f]
            place = plan[WORKING * SIDES + t * SIDES + f]
            for c, src in enumerate((ghosts, g_ym, g_yp, g_xm, g_xp, g_y2m, g_y2p)):
                pl.when(kind == c)(functools.partial(copy_face, ghost, f, src, place))
            return carry

        lax.fori_loop(0, SIDES, gather, 0)

        def prepare(load):
            def layer(x, carry):
                a, i, v, p, q = (load(s, x) for s in range(SPECIES))
                half = 0.5 * (a + p + q)
                electrons = half + jnp.sqrt(half * half + 1.0)
                pi = rate[0] * a * i - rate[1] * p
                pv = rate[2] * a * v - rate[3] * q
                re = rate[4] * (i * v - 1.0)
                source = (a - pi - pv, i - pi - re, v - pv - re, p + pi, q + pv)
                at = pl.multiple_of(x * PAD + TILES, 8)
                for s, value in enumerate((a, i, v, p, q)):
                    spread = flat[s] + slope[s] * electrons
                    inverse = 1.0 / (1.0 + 6.0 * spread)
                    grid[0, s, pl.ds(at, TILES), :] = value
                    fixed[s, x] = source[s] * inverse
                    factor[s, x] = spread * inverse
                return carry

            lax.fori_loop(0, B, layer, 0, unroll=2)

        pl.when(kind_of_patch == 0)(
            functools.partial(prepare, lambda s, x: dense_ref[place_of_patch, s, x])
        )
        for c, src in ((1, p_xm), (2, p_xp), (3, p_ym), (4, p_yp)):
            pl.when(kind_of_patch == c)(functools.partial(prepare, lambda s, x, src=src: src[s, x]))

        def one_species(s, carry, t=t):
            fixed[s, 0] = fixed[s, 0] + factor[s, 0] * ghost[0, s]
            fixed[s, B - 1] = fixed[s, B - 1] + factor[s, B - 1] * ghost[1, s]
            y_first, y_last = ghost[2, s], ghost[3, s]
            z_first, z_last = ghost[4, s], ghost[5, s]
            firsts = [pltpu.roll(y_first, (128 - j * B) % 128, 1) if j else y_first for j in range(4)]
            lasts = [pltpu.roll(y_last, (3 - j) * B, 1) if j < 3 else y_last for j in range(4)]
            for x in range(B):
                zf = pltpu.roll(z_first, 128 - x, 1) if x else z_first
                zl = pltpu.roll(z_last, B - 1 - x, 1) if x < B - 1 else z_last
                i, j = x // 4, x % 4
                yf = pltpu.roll(firsts[j], TILES - i, 0) if i else firsts[j]
                yl = pltpu.roll(lasts[j], TILES - 1 - i, 0) if i < TILES - 1 else lasts[j]
                outer = jnp.where(z_low, zf, jnp.where(z_high, zl, zero))
                outer = outer + jnp.where(y_low, yf, jnp.where(y_high, yl, zero))
                fixed[s, x] = fixed[s, x] + factor[s, x] * outer
            for sweep in range(SWEEPS):
                a, b = sweep % 2, (sweep + 1) % 2
                before = None
                here = grid[a, s, pl.ds(TILES, TILES), :]
                for x in range(B):
                    at = x * PAD + TILES
                    after = grid[a, s, pl.ds(at + PAD, TILES), :] if x < B - 1 else None
                    up = grid[a, s, pl.ds(at - 1, TILES), :]
                    down = grid[a, s, pl.ds(at + 1, TILES), :]
                    total = pltpu.roll(jnp.where(lane >= 128 - B, up, here), B, 1)
                    total = total + pltpu.roll(jnp.where(lane < B, down, here), 128 - B, 1)
                    total = total + jnp.where(z_low, zero, pltpu.roll(here, 1, 1))
                    total = total + jnp.where(z_high, zero, pltpu.roll(here, 127, 1))
                    if before is not None:
                        total = total + before
                    if after is not None:
                        total = total + after
                    new = fixed[s, x] + factor[s, x] * total
                    if sweep < SWEEPS - 1:
                        grid[b, s, pl.ds(at, TILES), :] = new
                    else:
                        row = s * (B * TILES * 8) + x * (TILES * 8) + t
                        stage_rows[pl.ds(row, TILES, stride=8), :] = new
                    before, here = here, after
            if t == WORKING - 1:
                copy_out(s).start()
            return carry

        def copy_out(s):
            return pltpu.make_async_copy(
                stage.at[s, :, pl.ds(0, cap), :], out_ref.at[s], sems.at[s]
            )

        def skip(s, carry, t=t):
            if t == WORKING - 1:
                copy_out(s).start()
            return carry

        live = kind_of_patch >= 0

        @pl.when(live)
        def _():
            lax.fori_loop(0, SPECIES, one_species, 0)

        if t == WORKING - 1:

            @pl.when(jnp.logical_not(live))
            def _():
                lax.fori_loop(0, SPECIES, skip, 0)

            for s in range(SPECIES):
                copy_out(s).wait()


def passed_along(x, axis, by):
    devices = lax.axis_size(axis)
    pairs = [(i, i + by) for i in range(devices) if 0 <= i + by < devices]
    return lax.ppermute(x, axis, pairs)


def both_ways(up, down, axis, by=1):
    return passed_along(up, axis, by), passed_along(down, axis, -by)


def shape(*dims):
    return jax.ShapeDtypeStruct(dims, F32)


def body(concentration, neighbours, source_slot, mobility, fermi_gain, rates):
    cap, species, cells = concentration.shape
    rows = lax.axis_size("gy")
    me = lax.axis_index("gx") * rows + lax.axis_index("gy")
    meta = Meta(cap)
    own = meta.build(neighbours, source_slot, me)
    view = concentration.reshape(cap, species, cells // 128, 128).transpose(1, 2, 0, 3)

    xm, xp = both_ways(own, own, "gx")
    y2m, y2p = both_ways(own, own, "gy", 2)
    strip = jnp.concatenate([own, xm, xp])
    ym, yp = both_ways(strip, strip, "gy")

    dense, faces = pl.pallas_call(
        functools.partial(pack_kernel, cap),
        out_shape=(shape(cap, species, B, *LAYER), shape(cap * SIDES, species, *LAYER)),
        in_specs=[ANY],
        out_specs=(VMEM, VMEM),
        scratch_shapes=[
            pltpu.VMEM((species, cells // 128, 8, 128), F32),
            pltpu.SemaphoreType.DMA((species,)),
        ],
        name="pack",
    )(view)
    f_xm, f_xp = both_ways(faces, faces, "gx")

    patch = shape(species, B, *LAYER)
    s_xp, s_xm, s_yp, s_ym = pl.pallas_call(
        functools.partial(patches_kernel, meta, rows),
        out_shape=(patch,) * 4,
        in_specs=[SMEM] * 5 + [VMEM],
        out_specs=(VMEM,) * 4,
        name="patches",
    )(own, xm, xp, ym, yp, dense)
    p_ym, p_yp = both_ways(s_yp, s_ym, "gy")
    p_xm, p_xp = both_ways(s_xp, s_xm, "gx")

    all_sides = shape(WORKING * SIDES, species, *LAYER)
    one_patch = shape(SIDES, species, *LAYER)
    t_yp, t_ym, t_xp, t_xm, t_y2p, t_y2m, ghosts, plan = pl.pallas_call(
        functools.partial(faces_kernel, meta, rows),
        out_shape=(all_sides,) * 2 + (one_patch,) * 4
        + (all_sides, jax.ShapeDtypeStruct((2 * WORKING * SIDES + 2 * WORKING,), jnp.int32)),
        in_specs=[SMEM] * 7 + [VMEM] * 3,
        out_specs=(VMEM,) * 7 + (SMEM,),
        name="faces",
    )(own, xm, xp, ym, yp, y2m, y2p, faces, f_xm, f_xp)
    g_ym, g_yp = both_ways(t_yp, t_ym, "gy")
    g_y2m, g_y2p = both_ways(t_y2p, t_y2m, "gy", 2)
    g_xm, g_xp = both_ways(t_xp, t_xm, "gx")

    moved = pl.pallas_call(
        functools.partial(sweep_kernel, cap),
        out_shape=shape(species, cells // 128, cap, 128),
        in_specs=[SMEM] * 4 + [VMEM] * 12,
        out_specs=ANY,
        scratch_shapes=[
            pltpu.VMEM((SIDES, species, *LAYER), F32),
            pltpu.VMEM((2, species, B * PAD + TILES, 128), F32),
            pltpu.VMEM((species, B, *LAYER), F32),
            pltpu.VMEM((species, B, *LAYER), F32),
            pltpu.VMEM((species, cells // 128, 8, 128), F32),
            pltpu.SemaphoreType.DMA((species,)),
        ],
        name="sweeps",
    )(plan, mobility, fermi_gain, rates, dense, p_xm, p_xp, p_ym, p_yp,
      ghosts, g_ym, g_yp, g_xm, g_xp, g_y2m, g_y2p)
    return moved.transpose(2, 0, 1, 3).reshape(cap, species, cells)


def solution(mesh):
    placed = (P(("gx", "gy"), None, None), P(("gx", "gy"), None), P(("gx", "gy")), P(), P(), P())
    return jax.shard_map(
        body, mesh=mesh, in_specs=placed, out_specs=P(("gx", "gy"), None, None), check_vma=False
    )
```

```python
import functools

import jax
import jax.numpy as jnp
from jax import lax
from jax.experimental import pallas as pl
from jax.experimental.pallas import tpu as pltpu
from jax.sharding import PartitionSpec as P


B = 32
SPECIES = 5
SWEEPS = 3
KEEP = 2
MOVE = 1
WORKING = KEEP - 1 + MOVE
SIDES = 6
TILES = B * B // 128
LAYER = (TILES, 128)
PAD = 2 * TILES


VMEM = pl.BlockSpec(memory_space=pltpu.VMEM)
SMEM = pl.BlockSpec(memory_space=pltpu.SMEM)
ANY = pl.BlockSpec(memory_space=pl.ANY)
F32 = jnp.float32
VMEM_LIMIT = 24 << 20


def iotas():
    sub = lax.broadcasted_iota(jnp.int32, LAYER, 0)
    lane = lax.broadcasted_iota(jnp.int32, LAYER, 1)
    return sub, lane


def raw_copy(c_ref, raw, sems, cap, s):
    return pltpu.make_async_copy(c_ref.at[s], raw.at[s, :, pl.ds(0, cap), :], sems.at[s])


def raw_rows(raw):
    return raw.reshape(SPECIES * B * TILES * 8, 128)


PER_X = TILES * 8
PER_S = B * PER_X


class Table:
    def __init__(self, cap, rows, devices):
        self.cap, self.rows, self.devices = cap, rows, devices
        self.width = -(-(1 + SIDES) * cap // 8) * 8
        self.scale = -(-(1 << 16) // cap)
        assert all((p * self.scale) >> 16 == p // cap for p in range(cap * devices))

    def gather(self, neighbours, source_slot):
        own = jnp.concatenate([source_slot, neighbours.reshape(-1)])
        own = jnp.pad(own, (0, self.width - own.shape[0]))
        sent = jnp.broadcast_to(own[None], (self.devices, self.width))
        return lax.all_to_all(sent, ("gx", "gy"), 0, 0, tiled=True).reshape(-1)

    def device(self, slot):
        return (slot * self.scale) >> 16

    def there(self, device):
        return jnp.clip(device, 0, self.devices - 1)

    def take(self, table, device, t):
        return table[self.there(device) * self.width + t]

    def local(self, slot, device):
        at = slot - device * self.cap
        return (at >= 0) & (at < self.cap), jnp.clip(at, 0, self.cap - 1)

    def need(self, table, slot, side):
        safe = jnp.maximum(slot, 0)
        home = self.device(safe)
        near = table[home * self.width + self.cap + (safe - home * self.cap) * SIDES + side]
        face = jnp.where(near < 0, side, side ^ 1)
        return jnp.where(slot < 0, -1, jnp.where(near < 0, slot, near)), face


def each_side(body):
    def step(f, carry):
        body(f)
        return carry

    lax.fori_loop(0, SIDES, step, 0)


def copy_face(dst, dst_at, src, src_at):
    for s in range(SPECIES):
        dst[dst_at, s] = src[src_at, s]


def picked(info, table, me, device):
    pick = jnp.int32(0)
    for t in range(WORKING):
        here, at = info.local(info.take(table, device, t), me)
        pick = jnp.where(here, at, pick)
    return pick


def pack_kernel(cap, c_ref, dense, faces, raw, sems):
    for s in range(SPECIES):
        raw_copy(c_ref, raw, sems, cap, s).start()
    rows = raw_rows(raw)
    _, lane = iotas()
    z = lane & (B - 1)
    quarter = lane // B

    def species(s, carry):
        raw_copy(c_ref, raw, sems, cap, s).wait()
        base = s * PER_S

        def slot(p, carry2):
            start = base + p
            z_first = z_last = None
            for x in range(B):
                v = rows[pl.ds(start + x * PER_X, TILES, stride=8), :]
                dense[p, s, x] = v
                a = v if x == 0 else pltpu.roll(v, x, 1)
                b = v if x == B - 1 else pltpu.roll(v, 128 + x - (B - 1), 1)
                z_first = a if x == 0 else jnp.where(z == x, a, z_first)
                z_last = b if x == 0 else jnp.where(z == x, b, z_last)
                if x == 0:
                    faces[p * SIDES + 0, s] = v
                if x == B - 1:
                    faces[p * SIDES + 1, s] = v
            y_first = y_last = None
            for j in range(4):
                a = rows[pl.ds(start + j * PER_X, TILES, stride=4 * PER_X), :]
                b = rows[pl.ds(start + j * PER_X + (TILES - 1) * 8, TILES, stride=4 * PER_X), :]
                a = a if j == 0 else pltpu.roll(a, j * B, 1)
                b = b if j == 3 else pltpu.roll(b, (j + 1) * B, 1)
                y_first = a if j == 0 else jnp.where(quarter == j, a, y_first)
                y_last = b if j == 0 else jnp.where(quarter == j, b, y_last)
            faces[p * SIDES + 2, s] = y_first
            faces[p * SIDES + 3, s] = y_last
            faces[p * SIDES + 4, s] = z_first
            faces[p * SIDES + 5, s] = z_last
            return carry2

        return lax.fori_loop(0, cap, slot, carry)

    lax.fori_loop(0, SPECIES, species, 0)


def copy_patches(pairs, dense):
    def layer(x, carry):
        for s in range(SPECIES):
            for number, out in pairs:
                out[s, x] = dense[number, s, x]
        return carry

    lax.fori_loop(0, B, layer, 0, unroll=4)


def first_kernel(info, me_ref, table, dense, to_yp, to_ym):
    me = me_ref[0]
    up, down = picked(info, table, me, me + 1), picked(info, table, me, me - 1)
    copy_patches(((up, to_yp), (down, to_ym)), dense)


def second_kernel(
    info, me_ref, table, dense, faces, to_xp, to_xm, to_x2p, to_x2m, to_y2p, to_y2m, patches
):
    me = me_ref[0]
    up, down = picked(info, table, me, me + info.rows), picked(info, table, me, me - info.rows)
    copy_patches(((up, to_xp), (down, to_xm)), dense)
    for t in range(WORKING):
        slot = info.take(table, me, t)
        kind = jnp.int32(-1)
        for c, device in enumerate((me, me - info.rows, me + info.rows, me - 1, me + 1)):
            kind = jnp.where((slot >= 0) & info.local(slot, device)[0], c, kind)
        patches[t] = kind
        patches[WORKING + t] = info.local(slot, me)[1]

    for step, out in ((info.rows, to_x2p), (-info.rows, to_x2m), (1, to_y2p), (-1, to_y2m)):
        for t in range(WORKING):
            slot = info.take(table, me + 2 * step, t)
            between, _ = info.local(slot, me + step)

            @pl.when(between)
            def _(slot=slot, out=out):
                @each_side
                def _(f):
                    near, face = info.need(table, slot, f)
                    here, at = info.local(near, me)
                    pl.when(here)(
                        functools.partial(copy_face, out, f, faces, at * SIDES + face)
                    )


def faces_kernel(info, me_ref, table, f_own, f_xm, f_xp, to_yp, to_ym, ghosts, plan):
    me = me_ref[0]
    shifts = ((0, f_own), (-info.rows, f_xm), (info.rows, f_xp))
    for step, out in ((1, to_yp), (-1, to_ym), (0, ghosts)):
        for t in range(WORKING):
            slot = info.take(table, me + step, t)

            @each_side
            def _(f, t=t, step=step, out=out, slot=slot):
                near, face = info.need(table, slot, f)
                at = t * SIDES + f
                for shift, src in shifts:
                    here, number = info.local(near, me + shift)
                    pl.when((near >= 0) & here)(
                        functools.partial(copy_face, out, at, src, number * SIDES + face)
                    )
                if step == 0:
                    home = info.device(jnp.maximum(near, 0))
                    column, my_column = home // info.rows, me // info.rows
                    row, my_row = home - column * info.rows, me - my_column * info.rows
                    beside = jnp.abs(column - my_column) < 2
                    kind, place = jnp.int32(0), at
                    kind = jnp.where(beside & (row == my_row - 1), 1, kind)
                    kind = jnp.where(beside & (row == my_row + 1), 2, kind)
                    for c, far in ((3, -2 * info.rows), (4, 2 * info.rows)):
                        kind = jnp.where(home == me + far, c, kind)
                    for c, far in ((5, -2), (6, 2)):
                        kind = jnp.where((column == my_column) & (row == my_row + far), c, kind)
                    place = jnp.where(kind > 2, f, place)
                    plan[at] = jnp.where(near >= 0, kind, 0)
                    plan[WORKING * SIDES + at] = place


def prepare_kernel(
    patches, mob, gain, rates, dense, p_xm, p_xp, p_ym, p_yp, grid, fixed, factor
):
    zero = jnp.zeros(LAYER, F32)

    def full(value):
        return jnp.full(LAYER, value, F32)

    flat, slope = [], []
    for s in range(SPECIES):
        m, g = full(mob[s]), full(gain[s])
        flat.append(m / (1.0 + g))
        slope.append(m * g / (1.0 + g))
    rate = [full(rates[i]) for i in range(5)]

    for t in range(WORKING):

        def prepare(load, t=t):
            def layer(x, carry):
                a, i, v, p, q = (load(s, x) for s in range(SPECIES))
                half = 0.5 * (a + p + q)
                electrons = half + jnp.sqrt(half * half + 1.0)
                pi = rate[0] * a * i - rate[1] * p
                pv = rate[2] * a * v - rate[3] * q
                re = rate[4] * (i * v - 1.0)
                source = (a - pi - pv, i - pi - re, v - pv - re, p + pi, q + pv)
                at = pl.multiple_of(x * PAD, 8)
                for s, value in enumerate((a, i, v, p, q)):
                    spread = flat[s] + slope[s] * electrons
                    inverse = 1.0 / (1.0 + 6.0 * spread)
                    grid[t, s, pl.ds(at, TILES), :] = zero
                    grid[t, s, pl.ds(at + TILES, TILES), :] = value
                    fixed[t, s, x] = source[s] * inverse
                    factor[t, s, x] = spread * inverse
                return carry

            lax.fori_loop(0, B, layer, 0, unroll=4)
            for s in range(SPECIES):
                grid[t, s, pl.ds(B * PAD, TILES), :] = zero

        kind = patches[t]
        pl.when(kind == 0)(
            functools.partial(prepare, lambda s, x, t=t: dense[patches[WORKING + t], s, x])
        )
        for c, src in ((1, p_xm), (2, p_xp), (3, p_ym), (4, p_yp)):
            pl.when(kind == c)(functools.partial(prepare, lambda s, x, src=src: src[s, x]))


def sweep_kernel(
    patches, plan, grid, fixed, factor, ghosts, g_ym, g_yp, g_xm, g_xp, g_y2m, g_y2p, blank,
    out_ref, ghost, mid, base, stage, sems,
):
    del blank
    sub, lane = iotas()
    z = lane & (B - 1)
    z_low, z_high = z == 0, z == B - 1
    y_low = (sub == 0) & (lane < B)
    y_high = (sub == TILES - 1) & (lane >= 128 - B)
    zero = jnp.zeros(LAYER, F32)
    stage_rows = raw_rows(stage)

    def clear_pad(i, carry):
        for a in range(2):
            mid[a, pl.ds(pl.multiple_of(i * PAD, 8), TILES), :] = zero
        return carry

    lax.fori_loop(0, B + 1, clear_pad, 0, unroll=3)

    def copy_out(s):
        return pltpu.make_async_copy(
            stage.at[s, :, pl.ds(0, WORKING), :],
            out_ref.at[s, :, pl.ds(0, WORKING), :],
            sems.at[s],
        )

    for t in range(WORKING):

        @each_side
        def _(f, t=t):
            kind = plan[t * SIDES + f]
            place = plan[WORKING * SIDES + t * SIDES + f]
            for c, src in enumerate((ghosts, g_ym, g_yp, g_xm, g_xp, g_y2m, g_y2p)):
                pl.when(kind == c)(functools.partial(copy_face, ghost, t * SIDES + f, src, place))

    def one_patch(t, s):
        at_side = t * SIDES
        y_first, y_last = ghost[at_side + 2, s], ghost[at_side + 3, s]
        z_first, z_last = ghost[at_side + 4, s], ghost[at_side + 5, s]
        firsts = [pltpu.roll(y_first, (128 - j * B) % 128, 1) if j else y_first for j in range(4)]
        lasts = [pltpu.roll(y_last, (3 - j) * B, 1) if j < 3 else y_last for j in range(4)]
        for x in range(B):
            zf = pltpu.roll(z_first, 128 - x, 1) if x else z_first
            zl = pltpu.roll(z_last, B - 1 - x, 1) if x < B - 1 else z_last
            i, j = x // 4, x % 4
            yf = pltpu.roll(firsts[j], TILES - i, 0) if i else firsts[j]
            yl = pltpu.roll(lasts[j], TILES - 1 - i, 0) if i < TILES - 1 else lasts[j]
            outer = jnp.where(z_low, zf, jnp.where(z_high, zl, zero))
            outer = outer + jnp.where(y_low, yf, jnp.where(y_high, yl, zero))
            if x == 0:
                outer = outer + ghost[at_side, s]
            if x == B - 1:
                outer = outer + ghost[at_side + 1, s]
            base[x] = fixed[t, s, x] + factor[t, s, x] * outer
        for sweep in range(SWEEPS):

            def load(row, sweep=sweep):
                if sweep == 0:
                    return grid[t, s, pl.ds(row, TILES), :]
                return mid[(sweep - 1) % 2, pl.ds(row, TILES), :]

            before = None
            here = load(TILES)
            for x in range(B):
                at = x * PAD + TILES
                after = load(at + PAD) if x < B - 1 else None
                total = pltpu.roll(jnp.where(lane >= 128 - B, load(at - 1), here), B, 1)
                total = total + pltpu.roll(jnp.where(lane < B, load(at + 1), here), 128 - B, 1)
                total = total + jnp.where(z_low, zero, pltpu.roll(here, 1, 1))
                total = total + jnp.where(z_high, zero, pltpu.roll(here, 127, 1))
                if before is not None:
                    total = total + before
                if after is not None:
                    total = total + after
                new = base[x] + factor[t, s, x] * total
                if sweep < SWEEPS - 1:
                    mid[sweep % 2, pl.ds(at, TILES), :] = new
                else:
                    stage_rows[pl.ds(s * PER_S + x * PER_X + t, TILES, stride=8), :] = new
                before, here = here, after

    def species(s, carry):
        for t in range(WORKING):
            live = patches[t] >= 0
            pl.when(live)(functools.partial(one_patch, t, s))

            @pl.when(jnp.logical_not(live))
            def _(t=t):
                for x in range(B):
                    stage_rows[pl.ds(s * PER_S + x * PER_X + t, TILES, stride=8), :] = zero

        copy_out(s).start()
        return carry

    lax.fori_loop(0, SPECIES, species, 0)
    for s in range(SPECIES):
        copy_out(s).wait()


def blank_kernel(cap, out_ref, zeros, sems):
    zeros[...] = jnp.zeros(zeros.shape, F32)

    def copy(s):
        return pltpu.make_async_copy(zeros.at[:, pl.ds(0, cap), :], out_ref.at[s], sems.at[s])

    for s in range(SPECIES):
        copy(s).start()
    for s in range(SPECIES):
        copy(s).wait()


def passed_along(x, axis, by):
    devices = lax.axis_size(axis)
    pairs = [(i, i + by) for i in range(devices) if 0 <= i + by < devices]
    return lax.ppermute(x, axis, pairs)


def both_ways(up, down, axis, by):
    return passed_along(up, axis, by), passed_along(down, axis, -by)


def call(kernel, out_shape, in_specs, out_specs, scratch=(), aliases=None):
    def run(*args):
        return pl.pallas_call(
            kernel,
            out_shape=out_shape,
            in_specs=in_specs,
            out_specs=out_specs,
            scratch_shapes=list(scratch),
            input_output_aliases=aliases or {},
            compiler_params=pltpu.CompilerParams(vmem_limit_bytes=VMEM_LIMIT),
        )(*args)

    return run


def shape(*dims, dtype=F32):
    return jax.ShapeDtypeStruct(dims, dtype)


def body(concentration, neighbours, source_slot, mobility, fermi_gain, rates):
    cap, species, cells = concentration.shape
    tiles = cells // 128
    rows, columns = lax.axis_size("gy"), lax.axis_size("gx")
    me = (lax.axis_index("gx") * rows + lax.axis_index("gy")).astype(jnp.int32)[None]
    info = Table(cap, rows, rows * columns)
    view = concentration.reshape(cap, species, tiles, 128).transpose(1, 2, 0, 3)
    table = info.gather(neighbours, source_slot)

    patch = shape(species, B, *LAYER)
    two_patches = shape(WORKING, species, B, *LAYER)
    all_sides = shape(WORKING * SIDES, species, *LAYER)
    one_patch = shape(SIDES, species, *LAYER)
    pack = call(
        functools.partial(pack_kernel, cap),
        (shape(cap, species, B, *LAYER), shape(cap * SIDES, species, *LAYER)),
        [ANY],
        (VMEM, VMEM),
        [pltpu.VMEM((species, tiles, 8, 128), F32), pltpu.SemaphoreType.DMA((species,))],
    )
    dense, faces = pack(view)
    blank = call(
        functools.partial(blank_kernel, cap),
        shape(species, tiles, cap, 128),
        [],
        ANY,
        [pltpu.VMEM((tiles, 8, 128), F32), pltpu.SemaphoreType.DMA((species,))],
    )()

    s_yp, s_ym = call(
        functools.partial(first_kernel, info), (patch,) * 2, [SMEM, SMEM, VMEM], (VMEM,) * 2
    )(me, table, dense)
    p_ym, p_yp = both_ways(s_yp, s_ym, "gy", 1)
    f_xm, f_xp = both_ways(faces, faces, "gx", 1)

    s_xp, s_xm, t_x2p, t_x2m, t_y2p, t_y2m, patches = call(
        functools.partial(second_kernel, info),
        (patch, patch) + (one_patch,) * 4 + (shape(2 * WORKING, dtype=jnp.int32),),
        [SMEM, SMEM, VMEM, VMEM],
        (VMEM,) * 6 + (SMEM,),
    )(me, table, dense, faces)
    p_xm, p_xp = both_ways(s_xp, s_xm, "gx", 1)

    t_yp, t_ym, ghosts, plan = call(
        functools.partial(faces_kernel, info),
        (all_sides,) * 3 + (shape(2 * WORKING * SIDES, dtype=jnp.int32),),
        [SMEM] * 2 + [VMEM] * 3,
        (VMEM,) * 3 + (SMEM,),
    )(me, table, faces, f_xm, f_xp)
    g_ym, g_yp = both_ways(t_yp, t_ym, "gy", 1)
    g_y2m, g_y2p = both_ways(t_y2p, t_y2m, "gy", 2)
    g_x2m, g_x2p = both_ways(t_x2p, t_x2m, "gx", 2)

    padded = shape(WORKING, species, B * PAD + TILES, 128)
    grid, fixed, factor = call(
        prepare_kernel, (padded, two_patches, two_patches), [SMEM] * 4 + [VMEM] * 5, (VMEM,) * 3
    )(patches, mobility, fermi_gain, rates, dense, p_xm, p_xp, p_ym, p_yp)

    moved = call(
        sweep_kernel,
        shape(species, tiles, cap, 128),
        [SMEM] * 2 + [VMEM] * 10 + [ANY],
        ANY,
        [
            pltpu.VMEM((WORKING * SIDES, species, *LAYER), F32),
            pltpu.VMEM((2, B * PAD + TILES, 128), F32),
            pltpu.VMEM((B, *LAYER), F32),
            pltpu.VMEM((species, tiles, 8, 128), F32),
            pltpu.SemaphoreType.DMA((species,)),
        ],
        {12: 0},
    )(patches, plan, grid, fixed, factor, ghosts, g_ym, g_yp, g_x2m, g_x2p, g_y2m, g_y2p, blank)
    return moved.transpose(2, 0, 1, 3).reshape(cap, species, cells)


def solution(mesh):
    placed = (P(("gx", "gy"), None, None), P(("gx", "gy"), None), P(("gx", "gy")), P(), P(), P())
    return jax.shard_map(
        body, mesh=mesh, in_specs=placed, out_specs=P(("gx", "gy"), None, None), check_vma=False
    )
```

```python
import functools

import jax
import jax.numpy as jnp
from jax import lax
from jax.experimental import pallas as pl
from jax.experimental.pallas import tpu as pltpu
from jax.sharding import PartitionSpec as P


B = 32
SPECIES = 5
SWEEPS = 3
KEEP = 2
MOVE = 1
WORKING = KEEP - 1 + MOVE
SIDES = 6
SPARE = 4
TILES = B * B // 128
LAYER = (TILES, 128)
PAD = 2 * TILES


VMEM = pl.BlockSpec(memory_space=pltpu.VMEM)
SMEM = pl.BlockSpec(memory_space=pltpu.SMEM)
ANY = pl.BlockSpec(memory_space=pl.ANY)
HBM = pl.BlockSpec(memory_space=pltpu.HBM)
F32 = jnp.float32


def iotas():
    sub = lax.broadcasted_iota(jnp.int32, LAYER, 0)
    lane = lax.broadcasted_iota(jnp.int32, LAYER, 1)
    return sub, lane


def raw_copy(c_ref, raw, sems, cap, s):
    return pltpu.make_async_copy(c_ref.at[s], raw.at[s, :, pl.ds(0, cap), :], sems.at[s])


def raw_rows(raw):
    return raw.reshape(SPECIES * B * TILES * 8, 128)


PER_X = TILES * 8
PER_S = B * PER_X


class Table:
    def __init__(self, cap, rows, devices):
        self.cap, self.rows, self.devices = cap, rows, devices
        self.width = -(-(1 + SIDES) * cap // 8) * 8
        self.scale = -(-(1 << 16) // cap)
        assert all((p * self.scale) >> 16 == p // cap for p in range(cap * devices))

    def gather(self, neighbours, source_slot):
        sent = call(
            functools.partial(table_kernel, self),
            shape(self.devices, 1, self.width, dtype=jnp.int32),
            [SMEM, SMEM],
            VMEM,
        )(source_slot, neighbours)
        return lax.all_to_all(sent, ("gx", "gy"), 0, 0, tiled=True)

    def device(self, slot):
        return (slot * self.scale) >> 16

    def there(self, device):
        return jnp.clip(device, 0, self.devices - 1)

    def take(self, table, device, t):
        return table[self.there(device), 0, t]

    def local(self, slot, device):
        at = slot - device * self.cap
        return (at >= 0) & (at < self.cap), jnp.clip(at, 0, self.cap - 1)

    def need(self, table, slot, side):
        safe = jnp.maximum(slot, 0)
        home = self.device(safe)
        near = table[home, 0, self.cap + (safe - home * self.cap) * SIDES + side]
        face = jnp.where(near < 0, side, side ^ 1)
        return jnp.where(slot < 0, -1, jnp.where(near < 0, slot, near)), face


def table_kernel(info, source_slot, neighbours, out):
    lane = lax.broadcasted_iota(jnp.int32, (1, info.width), 1)
    row = jnp.zeros((1, info.width), jnp.int32)
    for p in range(info.cap):
        row = jnp.where(lane == p, source_slot[p], row)
        for f in range(SIDES):
            row = jnp.where(lane == info.cap + p * SIDES + f, neighbours[p, f], row)
    for device in range(info.devices):
        out[device] = row


def each_side(body):
    def step(f, carry):
        body(f)
        return carry

    lax.fori_loop(0, SIDES, step, 0)


def copy_face(dst, dst_at, src, src_at):
    for s in range(SPECIES):
        dst[dst_at, s] = src[src_at, s]


def picked(info, table, me, device):
    pick = jnp.int32(0)
    for t in range(WORKING):
        here, at = info.local(info.take(table, device, t), me)
        pick = jnp.where(here, at, pick)
    return pick


def pack_kernel(cap, c_ref, dense_ref, faces, raw, dense, sems, out_sems):
    for s in range(SPECIES):
        raw_copy(c_ref, raw, sems, cap, s).start()
    rows = raw_rows(raw)
    _, lane = iotas()
    z = lane & (B - 1)
    quarter = lane // B

    def copy_out(s):
        return pltpu.make_async_copy(
            dense.at[:, s], dense_ref.at[pl.ds(0, cap), s], out_sems.at[s]
        )

    def species(s, carry):
        raw_copy(c_ref, raw, sems, cap, s).wait()
        base = s * PER_S

        for p in range(cap):
            start = base + p
            z_first = z_last = None
            for x in range(B):
                v = rows[pl.ds(start + x * PER_X, TILES, stride=8), :]
                dense[p, s, x] = v
                a = v if x == 0 else pltpu.roll(v, x, 1)
                b = v if x == B - 1 else pltpu.roll(v, 128 + x - (B - 1), 1)
                z_first = a if x == 0 else jnp.where(z == x, a, z_first)
                z_last = b if x == 0 else jnp.where(z == x, b, z_last)
                if x == 0:
                    faces[p * SIDES + 0, s] = v
                if x == B - 1:
                    faces[p * SIDES + 1, s] = v
            y_first = y_last = None
            for j in range(4):
                a = rows[pl.ds(start + j * PER_X, TILES, stride=4 * PER_X), :]
                b = rows[pl.ds(start + j * PER_X + (TILES - 1) * 8, TILES, stride=4 * PER_X), :]
                a = a if j == 0 else pltpu.roll(a, j * B, 1)
                b = b if j == 3 else pltpu.roll(b, (j + 1) * B, 1)
                y_first = a if j == 0 else jnp.where(quarter == j, a, y_first)
                y_last = b if j == 0 else jnp.where(quarter == j, b, y_last)
            faces[p * SIDES + 2, s] = y_first
            faces[p * SIDES + 3, s] = y_last
            faces[p * SIDES + 4, s] = z_first
            faces[p * SIDES + 5, s] = z_last
        copy_out(s).start()
        return carry

    lax.fori_loop(0, SPECIES, species, 0)
    for s in range(SPECIES):
        copy_out(s).wait()


def patch_copies(pairs, dense, sems):
    return [
        pltpu.make_async_copy(dense.at[number], out, sems.at[i])
        for i, (number, out) in enumerate(pairs)
    ]


def first_kernel(info, me_ref, table, dense, to_yp, to_ym, sems):
    me = me_ref[0]
    up, down = picked(info, table, me, me + 1), picked(info, table, me, me - 1)
    copies = patch_copies(((up, to_yp), (down, to_ym)), dense, sems)
    for copy in copies:
        copy.start()
    for copy in copies:
        copy.wait()


def second_kernel(
    info, me_ref, table, dense, faces, to_xp, to_xm, to_x2p, to_x2m, to_y2p, to_y2m, own, patches,
    sems,
):
    me = me_ref[0]
    up, down = picked(info, table, me, me + info.rows), picked(info, table, me, me - info.rows)
    kept = [info.local(info.take(table, me, t), me)[1] for t in range(WORKING)]
    pairs = [(up, to_xp), (down, to_xm), *((kept[t], own.at[t]) for t in range(WORKING))]
    copies = patch_copies(pairs, dense, sems)
    for copy in copies:
        copy.start()
    for t in range(WORKING):
        slot = info.take(table, me, t)
        kind = jnp.int32(-1)
        for c, device in enumerate((me, me - info.rows, me + info.rows, me - 1, me + 1)):
            kind = jnp.where((slot >= 0) & info.local(slot, device)[0], c, kind)
        patches[t] = kind

    for step, out in ((info.rows, to_x2p), (-info.rows, to_x2m), (1, to_y2p), (-1, to_y2m)):
        for t in range(WORKING):
            slot = info.take(table, me + 2 * step, t)
            between, _ = info.local(slot, me + step)

            @pl.when(between)
            def _(slot=slot, out=out):
                @each_side
                def _(f):
                    near, face = info.need(table, slot, f)
                    here, at = info.local(near, me)
                    pl.when(here)(
                        functools.partial(copy_face, out, f, faces, at * SIDES + face)
                    )

    for copy in copies:
        copy.wait()


def faces_kernel(info, me_ref, table, f_own, f_xm, f_xp, to_yp, to_ym, ghosts, plan):
    me = me_ref[0]
    shifts = ((0, f_own), (-info.rows, f_xm), (info.rows, f_xp))
    for step, out in ((1, to_yp), (-1, to_ym), (0, ghosts)):
        for t in range(WORKING):
            slot = info.take(table, me + step, t)

            @each_side
            def _(f, t=t, step=step, out=out, slot=slot):
                near, face = info.need(table, slot, f)
                at = t * SIDES + f
                for shift, src in shifts:
                    here, number = info.local(near, me + shift)
                    pl.when((near >= 0) & here)(
                        functools.partial(copy_face, out, at, src, number * SIDES + face)
                    )
                if step == 0:
                    home = info.device(jnp.maximum(near, 0))
                    column, my_column = home // info.rows, me // info.rows
                    row, my_row = home - column * info.rows, me - my_column * info.rows
                    beside = jnp.abs(column - my_column) < 2
                    kind, place = jnp.int32(0), at
                    kind = jnp.where(beside & (row == my_row - 1), 1, kind)
                    kind = jnp.where(beside & (row == my_row + 1), 2, kind)
                    for c, far in ((3, -2 * info.rows), (4, 2 * info.rows)):
                        kind = jnp.where(home == me + far, c, kind)
                    for c, far in ((5, -2), (6, 2)):
                        kind = jnp.where((column == my_column) & (row == my_row + far), c, kind)
                    place = jnp.where(kind > 2, f, place)
                    plan[at] = jnp.where(near >= 0, kind, 0)
                    plan[WORKING * SIDES + at] = place


def prepare_kernel(
    patches, mob, gain, rates, own, p_xm, p_xp, p_ym, p_yp, grid, fixed, factor
):
    zero = jnp.zeros(LAYER, F32)

    def full(value):
        return jnp.full(LAYER, value, F32)

    flat, slope = [], []
    for s in range(SPECIES):
        m, g = full(mob[s]), full(gain[s])
        flat.append(m / (1.0 + g))
        slope.append(m * g / (1.0 + g))
    rate = [full(rates[i]) for i in range(5)]

    for t in range(WORKING):

        def prepare(load, t=t):
            def layer(x, carry):
                a, i, v, p, q = (load(s, x) for s in range(SPECIES))
                half = 0.5 * (a + p + q)
                electrons = half + jnp.sqrt(half * half + 1.0)
                pi = rate[0] * a * i - rate[1] * p
                pv = rate[2] * a * v - rate[3] * q
                re = rate[4] * (i * v - 1.0)
                source = (a - pi - pv, i - pi - re, v - pv - re, p + pi, q + pv)
                at = pl.multiple_of(x * PAD, 8)
                for s, value in enumerate((a, i, v, p, q)):
                    spread = flat[s] + slope[s] * electrons
                    inverse = 1.0 / (1.0 + 6.0 * spread)
                    grid[t, s, pl.ds(at, TILES), :] = zero
                    grid[t, s, pl.ds(at + TILES, TILES), :] = value
                    fixed[t, s, x] = source[s] * inverse
                    factor[t, s, x] = spread * inverse
                return carry

            lax.fori_loop(0, B, layer, 0, unroll=4)
            for s in range(SPECIES):
                grid[t, s, pl.ds(B * PAD, TILES), :] = zero

        kind = patches[t]
        pl.when(kind == 0)(
            functools.partial(prepare, lambda s, x, t=t: own[t, s, x])
        )
        for c, src in ((1, p_xm), (2, p_xp), (3, p_ym), (4, p_yp)):
            pl.when(kind == c)(functools.partial(prepare, lambda s, x, src=src: src[s, x]))


def sweep_kernel(
    patches, plan, grid, fixed, factor, ghosts, g_ym, g_yp, g_xm, g_xp, g_y2m, g_y2p, blank,
    out_ref, ghost, mid, base, stage, sems,
):
    del blank
    sub, lane = iotas()
    z = lane & (B - 1)
    z_low, z_high = z == 0, z == B - 1
    y_low = (sub == 0) & (lane < B)
    y_high = (sub == TILES - 1) & (lane >= 128 - B)
    zero = jnp.zeros(LAYER, F32)
    stage_rows = raw_rows(stage)

    def clear_pad(i, carry):
        for a in range(2):
            mid[a, pl.ds(pl.multiple_of(i * PAD, 8), TILES), :] = zero
        return carry

    lax.fori_loop(0, B + 1, clear_pad, 0, unroll=3)

    def copy_out(s):
        return pltpu.make_async_copy(
            stage.at[s, :, pl.ds(0, WORKING), :],
            out_ref.at[s, :, pl.ds(0, WORKING), :],
            sems.at[s],
        )

    for t in range(WORKING):

        @each_side
        def _(f, t=t):
            kind = plan[t * SIDES + f]
            place = plan[WORKING * SIDES + t * SIDES + f]
            for c, src in enumerate((ghosts, g_ym, g_yp, g_xm, g_xp, g_y2m, g_y2p)):
                pl.when(kind == c)(functools.partial(copy_face, ghost, t * SIDES + f, src, place))

    def one_patch(t, s):
        at_side = t * SIDES
        y_first, y_last = ghost[at_side + 2, s], ghost[at_side + 3, s]
        z_first, z_last = ghost[at_side + 4, s], ghost[at_side + 5, s]
        firsts = [pltpu.roll(y_first, (128 - j * B) % 128, 1) if j else y_first for j in range(4)]
        lasts = [pltpu.roll(y_last, (3 - j) * B, 1) if j < 3 else y_last for j in range(4)]
        for x in range(B):
            zf = pltpu.roll(z_first, 128 - x, 1) if x else z_first
            zl = pltpu.roll(z_last, B - 1 - x, 1) if x < B - 1 else z_last
            i, j = x // 4, x % 4
            yf = pltpu.roll(firsts[j], TILES - i, 0) if i else firsts[j]
            yl = pltpu.roll(lasts[j], TILES - 1 - i, 0) if i < TILES - 1 else lasts[j]
            outer = jnp.where(z_low, zf, jnp.where(z_high, zl, zero))
            outer = outer + jnp.where(y_low, yf, jnp.where(y_high, yl, zero))
            if x == 0:
                outer = outer + ghost[at_side, s]
            if x == B - 1:
                outer = outer + ghost[at_side + 1, s]
            base[x] = fixed[t, s, x] + factor[t, s, x] * outer
        for sweep in range(SWEEPS):

            def load(row, sweep=sweep):
                if sweep == 0:
                    return grid[t, s, pl.ds(row, TILES), :]
                return mid[(sweep - 1) % 2, pl.ds(row, TILES), :]

            before = None
            here = load(TILES)
            for x in range(B):
                at = x * PAD + TILES
                after = load(at + PAD) if x < B - 1 else None
                total = pltpu.roll(jnp.where(lane >= 128 - B, load(at - 1), here), B, 1)
                total = total + pltpu.roll(jnp.where(lane < B, load(at + 1), here), 128 - B, 1)
                total = total + jnp.where(z_low, zero, pltpu.roll(here, 1, 1))
                total = total + jnp.where(z_high, zero, pltpu.roll(here, 127, 1))
                if before is not None:
                    total = total + before
                if after is not None:
                    total = total + after
                new = base[x] + factor[t, s, x] * total
                if sweep < SWEEPS - 1:
                    mid[sweep % 2, pl.ds(at, TILES), :] = new
                else:
                    stage_rows[pl.ds(s * PER_S + x * PER_X + t, TILES, stride=8), :] = new
                before, here = here, after

    def species(s, carry):
        for t in range(WORKING):
            live = patches[t] >= 0
            pl.when(live)(functools.partial(one_patch, t, s))

            @pl.when(jnp.logical_not(live))
            def _(t=t):
                for x in range(B):
                    stage_rows[pl.ds(s * PER_S + x * PER_X + t, TILES, stride=8), :] = zero

        copy_out(s).start()
        return carry

    lax.fori_loop(0, SPECIES, species, 0)
    for s in range(SPECIES):
        copy_out(s).wait()


def blank_kernel(cap, out_ref, zeros, sems):
    zeros[...] = jnp.zeros(zeros.shape, F32)

    def copy(s):
        return pltpu.make_async_copy(zeros.at[:, pl.ds(0, cap), :], out_ref.at[s], sems.at[s])

    for s in range(SPECIES):
        copy(s).start()
    for s in range(SPECIES):
        copy(s).wait()


def passed_along(x, axis, by):
    devices = lax.axis_size(axis)
    pairs = [(i, i + by) for i in range(devices) if 0 <= i + by < devices]
    return lax.ppermute(x, axis, pairs)


def both_ways(up, down, axis, by):
    return passed_along(up, axis, by), passed_along(down, axis, -by)


def call(kernel, out_shape, in_specs, out_specs, scratch=(), aliases=None, mib=2):
    def run(*args):
        return pl.pallas_call(
            kernel,
            out_shape=out_shape,
            in_specs=in_specs,
            out_specs=out_specs,
            scratch_shapes=list(scratch),
            input_output_aliases=aliases or {},
            compiler_params=pltpu.CompilerParams(vmem_limit_bytes=mib << 20),
        )(*args)

    return run


def shape(*dims, dtype=F32):
    return jax.ShapeDtypeStruct(dims, dtype)


def body(concentration, neighbours, source_slot, mobility, fermi_gain, rates):
    cap, species, cells = concentration.shape
    tiles = cells // 128
    rows, columns = lax.axis_size("gy"), lax.axis_size("gx")
    me = (lax.axis_index("gx") * rows + lax.axis_index("gy")).astype(jnp.int32)[None]
    info = Table(cap, rows, rows * columns)
    view = concentration.reshape(cap, species, tiles, 128).transpose(1, 2, 0, 3)
    table = info.gather(neighbours, source_slot)

    patch = shape(species, B, *LAYER)
    two_patches = shape(WORKING, species, B, *LAYER)
    all_sides = shape(WORKING * SIDES, species, *LAYER)
    one_patch = shape(SIDES, species, *LAYER)
    dense, faces = call(
        functools.partial(pack_kernel, cap),
        (shape(SPARE * cap, species, B, *LAYER), shape(cap * SIDES, species, *LAYER)),
        [HBM],
        (HBM, VMEM),
        [
            pltpu.VMEM((species, tiles, 8, 128), F32),
            pltpu.VMEM((cap, species, B, *LAYER), F32),
            pltpu.SemaphoreType.DMA((species,)),
            pltpu.SemaphoreType.DMA((species,)),
        ],
        mib=57,
    )(view)
    blank = call(
        functools.partial(blank_kernel, cap),
        shape(species, tiles, cap, 128),
        [],
        ANY,
        [pltpu.VMEM((tiles, 8, 128), F32), pltpu.SemaphoreType.DMA((species,))],
    )()

    s_yp, s_ym = call(
        functools.partial(first_kernel, info), (patch,) * 2, [SMEM, SMEM, HBM], (VMEM,) * 2,
        [pltpu.SemaphoreType.DMA((2,))],
        mib=50,
    )(me, table, dense)
    p_ym, p_yp = both_ways(s_yp, s_ym, "gy", 1)
    f_xm, f_xp = both_ways(faces, faces, "gx", 1)

    s_xp, s_xm, t_x2p, t_x2m, t_y2p, t_y2m, own, patches = call(
        functools.partial(second_kernel, info),
        (patch, patch) + (one_patch,) * 4 + (two_patches, shape(WORKING, dtype=jnp.int32)),
        [SMEM, SMEM, HBM, VMEM],
        (VMEM,) * 7 + (SMEM,),
        [pltpu.SemaphoreType.DMA((2 + WORKING,))],
        mib=50,
    )(me, table, dense, faces)
    p_xm, p_xp = both_ways(s_xp, s_xm, "gx", 1)

    t_yp, t_ym, ghosts, plan = call(
        functools.partial(faces_kernel, info),
        (all_sides,) * 3 + (shape(2 * WORKING * SIDES, dtype=jnp.int32),),
        [SMEM] * 2 + [VMEM] * 3,
        (VMEM,) * 3 + (SMEM,),
    )(me, table, faces, f_xm, f_xp)
    g_ym, g_yp = both_ways(t_yp, t_ym, "gy", 1)
    g_y2m, g_y2p = both_ways(t_y2p, t_y2m, "gy", 2)
    g_x2m, g_x2p = both_ways(t_x2p, t_x2m, "gx", 2)

    padded = shape(WORKING, species, B * PAD + TILES, 128)
    grid, fixed, factor = call(
        prepare_kernel, (padded, two_patches, two_patches), [SMEM] * 4 + [VMEM] * 5, (VMEM,) * 3
    )(patches, mobility, fermi_gain, rates, own, p_xm, p_xp, p_ym, p_yp)

    moved = call(
        sweep_kernel,
        shape(species, tiles, cap, 128),
        [SMEM] * 2 + [VMEM] * 10 + [ANY],
        ANY,
        [
            pltpu.VMEM((WORKING * SIDES, species, *LAYER), F32),
            pltpu.VMEM((2, B * PAD + TILES, 128), F32),
            pltpu.VMEM((B, *LAYER), F32),
            pltpu.VMEM((species, tiles, 8, 128), F32),
            pltpu.SemaphoreType.DMA((species,)),
        ],
        {12: 0},
        mib=10,
    )(patches, plan, grid, fixed, factor, ghosts, g_ym, g_yp, g_x2m, g_x2p, g_y2m, g_y2p, blank)
    return moved.transpose(2, 0, 1, 3).reshape(cap, species, cells)


def solution(mesh):
    placed = (P(("gx", "gy"), None, None), P(("gx", "gy"), None), P(("gx", "gy")), P(), P(), P())
    return jax.shard_map(
        body, mesh=mesh, in_specs=placed, out_specs=P(("gx", "gy"), None, None), check_vma=False
    )
```

```python
import functools

import jax
import jax.numpy as jnp
from jax import lax
from jax.experimental import pallas as pl
from jax.experimental.pallas import tpu as pltpu
from jax.sharding import PartitionSpec as P


B = 32
SPECIES = 5
SWEEPS = 3
KEEP = 2
MOVE = 1
WORKING = KEEP - 1 + MOVE
SIDES = 6
SPARE = 4
TILES = B * B // 128
LAYER = (TILES, 128)
PAD = 2 * TILES


VMEM = pl.BlockSpec(memory_space=pltpu.VMEM)
SMEM = pl.BlockSpec(memory_space=pltpu.SMEM)
ANY = pl.BlockSpec(memory_space=pl.ANY)
HBM = pl.BlockSpec(memory_space=pltpu.HBM)
F32 = jnp.float32


def iotas():
    sub = lax.broadcasted_iota(jnp.int32, LAYER, 0)
    lane = lax.broadcasted_iota(jnp.int32, LAYER, 1)
    return sub, lane


def raw_copy(c_ref, raw, sems, cap, s):
    return pltpu.make_async_copy(c_ref.at[s], raw.at[s, :, pl.ds(0, cap), :], sems.at[s])


def raw_rows(raw):
    return raw.reshape(SPECIES * B * TILES * 8, 128)


PER_X = TILES * 8
PER_S = B * PER_X


class Table:
    def __init__(self, cap, rows, devices):
        self.cap, self.rows, self.devices = cap, rows, devices
        self.width = -(-(1 + SIDES) * cap // 8) * 8
        self.scale = -(-(1 << 16) // cap)
        assert all((p * self.scale) >> 16 == p // cap for p in range(cap * devices))

    def gather(self, neighbours, source_slot):
        sent = call(
            functools.partial(table_kernel, self),
            shape(self.devices, 1, self.width, dtype=jnp.int32),
            [SMEM, SMEM],
            VMEM,
            mib=63,
        )(source_slot, neighbours)
        return lax.all_to_all(sent, ("gx", "gy"), 0, 0, tiled=True)

    def device(self, slot):
        return (slot * self.scale) >> 16

    def there(self, device):
        return jnp.clip(device, 0, self.devices - 1)

    def take(self, table, device, t):
        return table[self.there(device), 0, t]

    def local(self, slot, device):
        at = slot - device * self.cap
        return (at >= 0) & (at < self.cap), jnp.clip(at, 0, self.cap - 1)

    def need(self, table, slot, side):
        safe = jnp.maximum(slot, 0)
        home = self.device(safe)
        near = table[home, 0, self.cap + (safe - home * self.cap) * SIDES + side]
        face = jnp.where(near < 0, side, side ^ 1)
        return jnp.where(slot < 0, -1, jnp.where(near < 0, slot, near)), face


def table_kernel(info, source_slot, neighbours, out):
    lane = lax.broadcasted_iota(jnp.int32, (1, info.width), 1)
    row = jnp.zeros((1, info.width), jnp.int32)
    for p in range(info.cap):
        row = jnp.where(lane == p, source_slot[p], row)
        for f in range(SIDES):
            row = jnp.where(lane == info.cap + p * SIDES + f, neighbours[p, f], row)
    for device in range(info.devices):
        out[device] = row


def each_side(body):
    def step(f, carry):
        body(f)
        return carry

    lax.fori_loop(0, SIDES, step, 0)


def copy_face(dst, dst_at, src, src_at):
    for s in range(SPECIES):
        dst[dst_at, s] = src[src_at, s]


def picked(info, table, me, device):
    pick = jnp.int32(0)
    for t in range(WORKING):
        here, at = info.local(info.take(table, device, t), me)
        pick = jnp.where(here, at, pick)
    return pick


def pack_kernel(cap, c_ref, dense_ref, faces, raw, dense, sems, out_sems):
    for s in range(SPECIES):
        raw_copy(c_ref, raw, sems, cap, s).start()
    rows = raw_rows(raw)
    _, lane = iotas()
    z = lane & (B - 1)
    quarter = lane // B

    def copy_out(s):
        return pltpu.make_async_copy(
            dense.at[:, s], dense_ref.at[pl.ds(0, cap), s], out_sems.at[s]
        )

    def species(s, carry):
        raw_copy(c_ref, raw, sems, cap, s).wait()
        base = s * PER_S

        for p in range(cap):
            start = base + p
            z_first = z_last = None
            for x in range(B):
                v = rows[pl.ds(start + x * PER_X, TILES, stride=8), :]
                dense[p, s, x] = v
                a = v if x == 0 else pltpu.roll(v, x, 1)
                b = v if x == B - 1 else pltpu.roll(v, 128 + x - (B - 1), 1)
                z_first = a if x == 0 else jnp.where(z == x, a, z_first)
                z_last = b if x == 0 else jnp.where(z == x, b, z_last)
                if x == 0:
                    faces[p * SIDES + 0, s] = v
                if x == B - 1:
                    faces[p * SIDES + 1, s] = v
            y_first = y_last = None
            for j in range(4):
                a = rows[pl.ds(start + j * PER_X, TILES, stride=4 * PER_X), :]
                b = rows[pl.ds(start + j * PER_X + (TILES - 1) * 8, TILES, stride=4 * PER_X), :]
                a = a if j == 0 else pltpu.roll(a, j * B, 1)
                b = b if j == 3 else pltpu.roll(b, (j + 1) * B, 1)
                y_first = a if j == 0 else jnp.where(quarter == j, a, y_first)
                y_last = b if j == 0 else jnp.where(quarter == j, b, y_last)
            faces[p * SIDES + 2, s] = y_first
            faces[p * SIDES + 3, s] = y_last
            faces[p * SIDES + 4, s] = z_first
            faces[p * SIDES + 5, s] = z_last
        copy_out(s).start()
        return carry

    lax.fori_loop(0, SPECIES, species, 0)
    for s in range(SPECIES):
        copy_out(s).wait()


def patch_copies(pairs, dense, sems):
    return [
        pltpu.make_async_copy(dense.at[number], out, sems.at[i])
        for i, (number, out) in enumerate(pairs)
    ]


def first_kernel(info, me_ref, table, dense, to_yp, to_ym, sems):
    me = me_ref[0]
    up, down = picked(info, table, me, me + 1), picked(info, table, me, me - 1)
    copies = patch_copies(((up, to_yp), (down, to_ym)), dense, sems)
    for copy in copies:
        copy.start()
    for copy in copies:
        copy.wait()


def second_kernel(
    info, me_ref, table, dense, faces, to_xp, to_xm, to_x2p, to_x2m, to_y2p, to_y2m, own, patches,
    sems,
):
    me = me_ref[0]
    up, down = picked(info, table, me, me + info.rows), picked(info, table, me, me - info.rows)
    kept = [info.local(info.take(table, me, t), me)[1] for t in range(WORKING)]
    pairs = [(up, to_xp), (down, to_xm), *((kept[t], own.at[t]) for t in range(WORKING))]
    copies = patch_copies(pairs, dense, sems)
    for copy in copies:
        copy.start()
    for t in range(WORKING):
        slot = info.take(table, me, t)
        kind = jnp.int32(-1)
        for c, device in enumerate((me, me - info.rows, me + info.rows, me - 1, me + 1)):
            kind = jnp.where((slot >= 0) & info.local(slot, device)[0], c, kind)
        patches[t] = kind

    for step, out in ((info.rows, to_x2p), (-info.rows, to_x2m), (1, to_y2p), (-1, to_y2m)):
        for t in range(WORKING):
            slot = info.take(table, me + 2 * step, t)
            between, _ = info.local(slot, me + step)

            @pl.when(between)
            def _(slot=slot, out=out):
                @each_side
                def _(f):
                    near, face = info.need(table, slot, f)
                    here, at = info.local(near, me)
                    pl.when(here)(
                        functools.partial(copy_face, out, f, faces, at * SIDES + face)
                    )

    for copy in copies:
        copy.wait()


def faces_kernel(info, me_ref, table, f_own, f_xm, f_xp, to_yp, to_ym, ghosts, plan):
    me = me_ref[0]
    shifts = ((0, f_own), (-info.rows, f_xm), (info.rows, f_xp))
    for step, out in ((1, to_yp), (-1, to_ym), (0, ghosts)):
        for t in range(WORKING):
            slot = info.take(table, me + step, t)

            @each_side
            def _(f, t=t, step=step, out=out, slot=slot):
                near, face = info.need(table, slot, f)
                at = t * SIDES + f
                for shift, src in shifts:
                    here, number = info.local(near, me + shift)
                    pl.when((near >= 0) & here)(
                        functools.partial(copy_face, out, at, src, number * SIDES + face)
                    )
                if step == 0:
                    home = info.device(jnp.maximum(near, 0))
                    column, my_column = home // info.rows, me // info.rows
                    row, my_row = home - column * info.rows, me - my_column * info.rows
                    beside = jnp.abs(column - my_column) < 2
                    kind, place = jnp.int32(0), at
                    kind = jnp.where(beside & (row == my_row - 1), 1, kind)
                    kind = jnp.where(beside & (row == my_row + 1), 2, kind)
                    for c, far in ((3, -2 * info.rows), (4, 2 * info.rows)):
                        kind = jnp.where(home == me + far, c, kind)
                    for c, far in ((5, -2), (6, 2)):
                        kind = jnp.where((column == my_column) & (row == my_row + far), c, kind)
                    place = jnp.where(kind > 2, f, place)
                    plan[at] = jnp.where(near >= 0, kind, 0)
                    plan[WORKING * SIDES + at] = place


def prepare_kernel(
    patches, mob, gain, rates, own, p_xm, p_xp, p_ym, p_yp, grid, fixed, factor
):
    zero = jnp.zeros(LAYER, F32)

    def full(value):
        return jnp.full(LAYER, value, F32)

    flat, slope = [], []
    for s in range(SPECIES):
        m, g = full(mob[s]), full(gain[s])
        flat.append(m / (1.0 + g))
        slope.append(m * g / (1.0 + g))
    rate = [full(rates[i]) for i in range(5)]

    for t in range(WORKING):

        def prepare(load, t=t):
            def layer(x, carry):
                a, i, v, p, q = (load(s, x) for s in range(SPECIES))
                half = 0.5 * (a + p + q)
                electrons = half + jnp.sqrt(half * half + 1.0)
                pi = rate[0] * a * i - rate[1] * p
                pv = rate[2] * a * v - rate[3] * q
                re = rate[4] * (i * v - 1.0)
                source = (a - pi - pv, i - pi - re, v - pv - re, p + pi, q + pv)
                at = pl.multiple_of(x * PAD, 8)
                for s, value in enumerate((a, i, v, p, q)):
                    spread = flat[s] + slope[s] * electrons
                    inverse = 1.0 / (1.0 + 6.0 * spread)
                    grid[t, s, pl.ds(at, TILES), :] = zero
                    grid[t, s, pl.ds(at + TILES, TILES), :] = value
                    fixed[t, s, x] = source[s] * inverse
                    factor[t, s, x] = spread * inverse
                return carry

            lax.fori_loop(0, B, layer, 0, unroll=4)
            for s in range(SPECIES):
                grid[t, s, pl.ds(B * PAD, TILES), :] = zero

        kind = patches[t]
        pl.when(kind == 0)(
            functools.partial(prepare, lambda s, x, t=t: own[t, s, x])
        )
        for c, src in ((1, p_xm), (2, p_xp), (3, p_ym), (4, p_yp)):
            pl.when(kind == c)(functools.partial(prepare, lambda s, x, src=src: src[s, x]))


def stencil():
    source = lax.broadcasted_iota(jnp.int32, (256, 128), 0)
    target = lax.broadcasted_iota(jnp.int32, (256, 128), 1)
    inside = source < 128
    step = jnp.abs(source - target)
    along_z = (step == 1) & (source // B == target // B)
    across = jnp.abs(source - 128 - target) == 128 - B
    hit = (inside & (along_z | (step == B))) | (jnp.logical_not(inside) & across)
    return jnp.where(hit, 1.0, 0.0).astype(jnp.bfloat16)


def sweep_kernel(
    patches, plan, grid, fixed, factor, ghosts, g_ym, g_yp, g_xm, g_xp, g_y2m, g_y2p, blank,
    out_ref, ghost, mid_0, mid_1, base_0, base_1, weights, stage, sems,
):
    del blank
    mids, bases = (mid_0, mid_1), (base_0, base_1)
    sub, lane = iotas()
    z = lane & (B - 1)
    z_low, z_high = z == 0, z == B - 1
    y_low = (sub == 0) & (lane < B)
    y_high = (sub == TILES - 1) & (lane >= 128 - B)
    zero = jnp.zeros(LAYER, F32)
    stage_rows = raw_rows(stage)
    weights[...] = stencil()

    def clear_pad(i, carry):
        for mid in mids:
            for a in range(2):
                mid[a, pl.ds(pl.multiple_of(i * PAD, 8), TILES), :] = zero
        return carry

    lax.fori_loop(0, B + 1, clear_pad, 0, unroll=3)

    def copy_out(s):
        return pltpu.make_async_copy(
            stage.at[s, :, pl.ds(0, WORKING), :],
            out_ref.at[s, :, pl.ds(0, WORKING), :],
            sems.at[s],
        )

    for t in range(WORKING):

        @each_side
        def _(f, t=t):
            kind = plan[t * SIDES + f]
            place = plan[WORKING * SIDES + t * SIDES + f]
            for c, src in enumerate((ghosts, g_ym, g_yp, g_xm, g_xp, g_y2m, g_y2p)):
                pl.when(kind == c)(functools.partial(copy_face, ghost, t * SIDES + f, src, place))

    def add_ghosts(t, s):
        at_side = t * SIDES
        y_first, y_last = ghost[at_side + 2, s], ghost[at_side + 3, s]
        z_first, z_last = ghost[at_side + 4, s], ghost[at_side + 5, s]
        firsts = [pltpu.roll(y_first, (128 - j * B) % 128, 1) if j else y_first for j in range(4)]
        lasts = [pltpu.roll(y_last, (3 - j) * B, 1) if j < 3 else y_last for j in range(4)]
        for x in range(B):
            zf = pltpu.roll(z_first, 128 - x, 1) if x else z_first
            zl = pltpu.roll(z_last, B - 1 - x, 1) if x < B - 1 else z_last
            i, j = x // 4, x % 4
            yf = pltpu.roll(firsts[j], TILES - i, 0) if i else firsts[j]
            yl = pltpu.roll(lasts[j], TILES - 1 - i, 0) if i < TILES - 1 else lasts[j]
            outer = jnp.where(z_low, zf, jnp.where(z_high, zl, zero))
            outer = outer + jnp.where(y_low, yf, jnp.where(y_high, yl, zero))
            if x == 0:
                outer = outer + ghost[at_side, s]
            if x == B - 1:
                outer = outer + ghost[at_side + 1, s]
            bases[t][x] = fixed[t, s, x] + factor[t, s, x] * outer

    def loader(t, s, sweep):
        def load(row):
            if sweep == 0:
                return grid[t, s, pl.ds(row, TILES), :]
            return mids[t][(sweep - 1) % 2, pl.ds(row, TILES), :]

        return load

    def by_matmul(load):
        layers = []
        for x in range(B):
            at = x * PAD + TILES
            other = jnp.where(lane >= 64, load(at - 1), load(at + 1))
            layers.append(jnp.concatenate([load(at), other], axis=1))
        whole = jnp.concatenate(layers, axis=0)
        high = whole.astype(jnp.bfloat16)
        low = (whole - high.astype(F32)).astype(jnp.bfloat16)
        w = weights[...]
        sums = jnp.dot(high, w, preferred_element_type=F32)
        sums = sums + jnp.dot(low, w, preferred_element_type=F32)
        return [sums[x * TILES : (x + 1) * TILES] for x in range(B)]

    def by_rolls(load, x, here):
        at = x * PAD + TILES
        total = pltpu.roll(jnp.where(lane >= 128 - B, load(at - 1), here), B, 1)
        total = total + pltpu.roll(jnp.where(lane < B, load(at + 1), here), 128 - B, 1)
        total = total + jnp.where(z_low, zero, pltpu.roll(here, 1, 1))
        return total + jnp.where(z_high, zero, pltpu.roll(here, 127, 1))

    def one_sweep(t, s, sweep, sums, live):
        load = loader(t, s, sweep)
        before, here = None, load(TILES)
        for x in range(B):
            at = x * PAD + TILES
            after = load(at + PAD) if x < B - 1 else None
            total = by_rolls(load, x, here) if sums is None else sums[x]
            if before is not None:
                total = total + before
            if after is not None:
                total = total + after
            new = bases[t][x] + factor[t, s, x] * total
            if sweep < SWEEPS - 1:
                mids[t][sweep % 2, pl.ds(at, TILES), :] = new
            else:
                row = s * PER_S + x * PER_X + t
                stage_rows[pl.ds(row, TILES, stride=8), :] = jnp.where(live, new, zero)
            before, here = here, after

    lives = [jnp.full(LAYER, patches[t], jnp.int32) >= 0 for t in range(WORKING)]

    def species(s, carry):
        for t in range(WORKING):
            add_ghosts(t, s)
        for sweep in range(SWEEPS):
            for t in range(WORKING):
                sums = by_matmul(loader(t, s, sweep)) if t % 2 else None
                one_sweep(t, s, sweep, sums, lives[t])
        copy_out(s).start()
        return carry

    lax.fori_loop(0, SPECIES, species, 0)
    for s in range(SPECIES):
        copy_out(s).wait()


def blank_kernel(cap, out_ref, zeros, sems):
    zeros[...] = jnp.zeros(zeros.shape, F32)

    def copy(s):
        return pltpu.make_async_copy(zeros.at[:, pl.ds(0, cap), :], out_ref.at[s], sems.at[s])

    for s in range(SPECIES):
        copy(s).start()
    for s in range(SPECIES):
        copy(s).wait()


def passed_along(x, axis, by):
    devices = lax.axis_size(axis)
    pairs = [(i, i + by) for i in range(devices) if 0 <= i + by < devices]
    return lax.ppermute(x, axis, pairs)


def both_ways(up, down, axis, by):
    return passed_along(up, axis, by), passed_along(down, axis, -by)


def call(kernel, out_shape, in_specs, out_specs, scratch=(), aliases=None, mib=2):
    def run(*args):
        return pl.pallas_call(
            kernel,
            out_shape=out_shape,
            in_specs=in_specs,
            out_specs=out_specs,
            scratch_shapes=list(scratch),
            input_output_aliases=aliases or {},
            compiler_params=pltpu.CompilerParams(vmem_limit_bytes=mib << 20),
        )(*args)

    return run


def shape(*dims, dtype=F32):
    return jax.ShapeDtypeStruct(dims, dtype)


def body(concentration, neighbours, source_slot, mobility, fermi_gain, rates):
    cap, species, cells = concentration.shape
    tiles = cells // 128
    rows, columns = lax.axis_size("gy"), lax.axis_size("gx")
    me = (lax.axis_index("gx") * rows + lax.axis_index("gy")).astype(jnp.int32)[None]
    info = Table(cap, rows, rows * columns)
    view = concentration.reshape(cap, species, tiles, 128).transpose(1, 2, 0, 3)
    table = info.gather(neighbours, source_slot)

    patch = shape(species, B, *LAYER)
    two_patches = shape(WORKING, species, B, *LAYER)
    all_sides = shape(WORKING * SIDES, species, *LAYER)
    one_patch = shape(SIDES, species, *LAYER)
    dense, faces = call(
        functools.partial(pack_kernel, cap),
        (shape(SPARE * cap, species, B, *LAYER), shape(cap * SIDES, species, *LAYER)),
        [HBM],
        (HBM, VMEM),
        [
            pltpu.VMEM((species, tiles, 8, 128), F32),
            pltpu.VMEM((cap, species, B, *LAYER), F32),
            pltpu.SemaphoreType.DMA((species,)),
            pltpu.SemaphoreType.DMA((species,)),
        ],
        mib=57,
    )(view)
    blank = call(
        functools.partial(blank_kernel, cap),
        shape(species, tiles, cap, 128),
        [],
        ANY,
        [pltpu.VMEM((tiles, 8, 128), F32), pltpu.SemaphoreType.DMA((species,))],
    )()

    s_yp, s_ym = call(
        functools.partial(first_kernel, info), (patch,) * 2, [SMEM, SMEM, HBM], (VMEM,) * 2,
        [pltpu.SemaphoreType.DMA((2,))],
        mib=50,
    )(me, table, dense)
    p_ym, p_yp = both_ways(s_yp, s_ym, "gy", 1)
    f_xm, f_xp = both_ways(faces, faces, "gx", 1)

    s_xp, s_xm, t_x2p, t_x2m, t_y2p, t_y2m, own, patches = call(
        functools.partial(second_kernel, info),
        (patch, patch) + (one_patch,) * 4 + (two_patches, shape(WORKING, dtype=jnp.int32)),
        [SMEM, SMEM, HBM, VMEM],
        (VMEM,) * 7 + (SMEM,),
        [pltpu.SemaphoreType.DMA((2 + WORKING,))],
        mib=50,
    )(me, table, dense, faces)
    p_xm, p_xp = both_ways(s_xp, s_xm, "gx", 1)

    t_yp, t_ym, ghosts, plan = call(
        functools.partial(faces_kernel, info),
        (all_sides,) * 3 + (shape(2 * WORKING * SIDES, dtype=jnp.int32),),
        [SMEM] * 2 + [VMEM] * 3,
        (VMEM,) * 3 + (SMEM,),
    )(me, table, faces, f_xm, f_xp)
    g_ym, g_yp = both_ways(t_yp, t_ym, "gy", 1)
    g_y2m, g_y2p = both_ways(t_y2p, t_y2m, "gy", 2)
    g_x2m, g_x2p = both_ways(t_x2p, t_x2m, "gx", 2)

    padded = shape(WORKING, species, B * PAD + TILES, 128)
    grid, fixed, factor = call(
        prepare_kernel, (padded, two_patches, two_patches), [SMEM] * 4 + [VMEM] * 5, (VMEM,) * 3
    )(patches, mobility, fermi_gain, rates, own, p_xm, p_xp, p_ym, p_yp)

    moved = call(
        sweep_kernel,
        shape(species, tiles, cap, 128),
        [SMEM] * 2 + [VMEM] * 10 + [ANY],
        ANY,
        [
            pltpu.VMEM((WORKING * SIDES, species, *LAYER), F32),
            pltpu.VMEM((2, B * PAD + TILES, 128), F32),
            pltpu.VMEM((2, B * PAD + TILES, 128), F32),
            pltpu.VMEM((B, *LAYER), F32),
            pltpu.VMEM((B, *LAYER), F32),
            pltpu.VMEM((256, 128), jnp.bfloat16),
            pltpu.VMEM((species, tiles, 8, 128), F32),
            pltpu.SemaphoreType.DMA((species,)),
        ],
        {12: 0},
        mib=10,
    )(patches, plan, grid, fixed, factor, ghosts, g_ym, g_yp, g_x2m, g_x2p, g_y2m, g_y2p, blank)
    return moved.transpose(2, 0, 1, 3).reshape(cap, species, cells)


def solution(mesh):
    placed = (P(("gx", "gy"), None, None), P(("gx", "gy"), None), P(("gx", "gy")), P(), P(), P())
    return jax.shard_map(
        body, mesh=mesh, in_specs=placed, out_specs=P(("gx", "gy"), None, None), check_vma=False
    )
```

```python
import functools

import jax
import jax.numpy as jnp
from jax import lax
from jax.experimental import pallas as pl
from jax.experimental.pallas import tpu as pltpu
from jax.sharding import PartitionSpec as P


B = 32
SPECIES = 5
SWEEPS = 3
KEEP = 2
MOVE = 1
WORKING = KEEP - 1 + MOVE
SIDES = 6
SPARE = 4
TILES = B * B // 128
LAYER = (TILES, 128)
PAD = 2 * TILES


VMEM = pl.BlockSpec(memory_space=pltpu.VMEM)
SMEM = pl.BlockSpec(memory_space=pltpu.SMEM)
ANY = pl.BlockSpec(memory_space=pl.ANY)
HBM = pl.BlockSpec(memory_space=pltpu.HBM)
F32 = jnp.float32


def iotas():
    sub = lax.broadcasted_iota(jnp.int32, LAYER, 0)
    lane = lax.broadcasted_iota(jnp.int32, LAYER, 1)
    return sub, lane


def raw_copy(c_ref, raw, sems, cap, s):
    return pltpu.make_async_copy(c_ref.at[s], raw.at[s, :, pl.ds(0, cap), :], sems.at[s])


def raw_rows(raw):
    return raw.reshape(SPECIES * B * TILES * 8, 128)


PER_X = TILES * 8
PER_S = B * PER_X


class Table:
    def __init__(self, cap, rows, devices):
        self.cap, self.rows, self.devices = cap, rows, devices
        self.width = -(-(1 + SIDES) * cap // 8) * 8
        self.scale = -(-(1 << 16) // cap)
        assert all((p * self.scale) >> 16 == p // cap for p in range(cap * devices))

    def gather(self, neighbours, source_slot):
        sent = call(
            functools.partial(table_kernel, self),
            shape(self.devices, 1, self.width, dtype=jnp.int32),
            [SMEM, SMEM],
            VMEM,
            mib=63,
        )(source_slot, neighbours)
        return lax.all_to_all(sent, ("gx", "gy"), 0, 0, tiled=True)

    def device(self, slot):
        return (slot * self.scale) >> 16

    def there(self, device):
        return jnp.clip(device, 0, self.devices - 1)

    def take(self, table, device, t):
        return table[self.there(device), 0, t]

    def local(self, slot, device):
        at = slot - device * self.cap
        return (at >= 0) & (at < self.cap), jnp.clip(at, 0, self.cap - 1)

    def need(self, table, slot, side):
        safe = jnp.maximum(slot, 0)
        home = self.device(safe)
        near = table[home, 0, self.cap + (safe - home * self.cap) * SIDES + side]
        face = jnp.where(near < 0, side, side ^ 1)
        return jnp.where(slot < 0, -1, jnp.where(near < 0, slot, near)), face


def table_kernel(info, source_slot, neighbours, out):
    lane = lax.broadcasted_iota(jnp.int32, (1, info.width), 1)
    row = jnp.zeros((1, info.width), jnp.int32)
    for p in range(info.cap):
        row = jnp.where(lane == p, source_slot[p], row)
        for f in range(SIDES):
            row = jnp.where(lane == info.cap + p * SIDES + f, neighbours[p, f], row)
    for device in range(info.devices):
        out[device] = row


def each_side(body):
    def step(f, carry):
        body(f)
        return carry

    lax.fori_loop(0, SIDES, step, 0)


def copy_face(dst, dst_at, src, src_at):
    for s in range(SPECIES):
        dst[dst_at, s] = src[src_at, s]


def picked(info, table, me, device):
    pick = jnp.int32(0)
    for t in range(WORKING):
        here, at = info.local(info.take(table, device, t), me)
        pick = jnp.where(here, at, pick)
    return pick


def pack_kernel(cap, c_ref, dense_ref, faces, raw, dense, sems, out_sems):
    for s in range(SPECIES):
        raw_copy(c_ref, raw, sems, cap, s).start()
    rows = raw_rows(raw)
    _, lane = iotas()
    z = lane & (B - 1)
    quarter = lane // B

    def copy_out(s):
        return pltpu.make_async_copy(
            dense.at[:, s], dense_ref.at[pl.ds(0, cap), s], out_sems.at[s]
        )

    def species(s, carry):
        raw_copy(c_ref, raw, sems, cap, s).wait()
        base = s * PER_S

        for p in range(cap):
            start = base + p
            z_first = z_last = None
            for x in range(B):
                v = rows[pl.ds(start + x * PER_X, TILES, stride=8), :]
                dense[p, s, x] = v
                a = v if x == 0 else pltpu.roll(v, x, 1)
                b = v if x == B - 1 else pltpu.roll(v, 128 + x - (B - 1), 1)
                z_first = a if x == 0 else jnp.where(z == x, a, z_first)
                z_last = b if x == 0 else jnp.where(z == x, b, z_last)
                if x == 0:
                    faces[p * SIDES + 0, s] = v
                if x == B - 1:
                    faces[p * SIDES + 1, s] = v
            y_first = y_last = None
            for j in range(4):
                a = rows[pl.ds(start + j * PER_X, TILES, stride=4 * PER_X), :]
                b = rows[pl.ds(start + j * PER_X + (TILES - 1) * 8, TILES, stride=4 * PER_X), :]
                a = a if j == 0 else pltpu.roll(a, j * B, 1)
                b = b if j == 3 else pltpu.roll(b, (j + 1) * B, 1)
                y_first = a if j == 0 else jnp.where(quarter == j, a, y_first)
                y_last = b if j == 0 else jnp.where(quarter == j, b, y_last)
            faces[p * SIDES + 2, s] = y_first
            faces[p * SIDES + 3, s] = y_last
            faces[p * SIDES + 4, s] = z_first
            faces[p * SIDES + 5, s] = z_last
        copy_out(s).start()
        return carry

    lax.fori_loop(0, SPECIES, species, 0)
    for s in range(SPECIES):
        copy_out(s).wait()


def patch_copies(pairs, dense, sems):
    return [
        pltpu.make_async_copy(dense.at[number], out, sems.at[i])
        for i, (number, out) in enumerate(pairs)
    ]


def first_kernel(info, me_ref, table, dense, to_yp, to_ym, sems):
    me = me_ref[0]
    up, down = picked(info, table, me, me + 1), picked(info, table, me, me - 1)
    copies = patch_copies(((up, to_yp), (down, to_ym)), dense, sems)
    for copy in copies:
        copy.start()
    for copy in copies:
        copy.wait()


def plan_sides(info, me, table, plan):
    my_column = me // info.rows
    my_row = me - my_column * info.rows
    for t in range(WORKING):
        slot = info.take(table, me, t)

        @each_side
        def _(f, t=t, slot=slot):
            near, face = info.need(table, slot, f)
            at = t * SIDES + f
            safe = jnp.maximum(near, 0)
            home = info.device(safe)
            column = home // info.rows
            row = home - column * info.rows
            beside = jnp.abs(column - my_column) < 2
            here = (safe - home * info.cap) * SIDES + face
            kind, place = jnp.int32(0), here
            for c, far in ((7, -info.rows), (8, info.rows)):
                kind = jnp.where(home == me + far, c, kind)
            for c, far in ((1, -1), (2, 1)):
                hit = beside & (row == my_row + far)
                kind, place = jnp.where(hit, c, kind), jnp.where(hit, at, place)
            for c, far in ((3, -2 * info.rows), (4, 2 * info.rows)):
                hit = home == me + far
                kind, place = jnp.where(hit, c, kind), jnp.where(hit, f, place)
            for c, far in ((5, -2), (6, 2)):
                hit = (column == my_column) & (row == my_row + far)
                kind, place = jnp.where(hit, c, kind), jnp.where(hit, f, place)
            plan[at] = jnp.where(near >= 0, kind, 0)
            plan[WORKING * SIDES + at] = jnp.where(near >= 0, place, 0)


def second_kernel(info, me_ref, table, dense, faces, *refs):
    to_xp, to_xm, to_x2p, to_x2m, to_y2p, to_y2m, own, sems = refs
    me = me_ref[0]
    up, down = picked(info, table, me, me + info.rows), picked(info, table, me, me - info.rows)
    kept = [info.local(info.take(table, me, t), me)[1] for t in range(WORKING)]
    pairs = [(up, to_xp), (down, to_xm), *((kept[t], own.at[t]) for t in range(WORKING))]
    copies = patch_copies(pairs, dense, sems)
    for copy in copies:
        copy.start()

    for step, out in ((info.rows, to_x2p), (-info.rows, to_x2m), (1, to_y2p), (-1, to_y2m)):
        for t in range(WORKING):
            slot = info.take(table, me + 2 * step, t)
            between, _ = info.local(slot, me + step)

            @pl.when(between)
            def _(slot=slot, out=out):
                @each_side
                def _(f):
                    near, face = info.need(table, slot, f)
                    here, at = info.local(near, me)
                    pl.when(here)(
                        functools.partial(copy_face, out, f, faces, at * SIDES + face)
                    )

    for copy in copies:
        copy.wait()


def copy_row(info, me, near, face, out, at, f_own, f_xm, f_xp):
    for shift, src in ((0, f_own), (-info.rows, f_xm), (info.rows, f_xp)):
        here, number = info.local(near, me + shift)
        pl.when((near >= 0) & here)(
            functools.partial(copy_face, out, at, src, number * SIDES + face)
        )


def faces_kernel(info, me_ref, table, f_own, f_xm, f_xp, to_yp, to_ym):
    me = me_ref[0]
    for step, out in ((1, to_yp), (-1, to_ym)):
        for t in range(WORKING):
            slot = info.take(table, me + step, t)

            @each_side
            def _(f, t=t, out=out, slot=slot):
                near, face = info.need(table, slot, f)
                copy_row(info, me, near, face, out, t * SIDES + f, f_own, f_xm, f_xp)


def prepare_kernel(
    info, me_ref, table, mob, gain, rates, own, p_xm, p_xp, p_ym, p_yp,
    grid, fixed, factor, patches, plan, blank, zeros, sems,
):
    zeros[...] = jnp.zeros(zeros.shape, F32)
    copies = [
        pltpu.make_async_copy(zeros.at[:, pl.ds(0, info.cap), :], blank.at[s], sems.at[s])
        for s in range(SPECIES)
    ]
    for copy in copies:
        copy.start()
    me = me_ref[0]
    for t in range(WORKING):
        slot = info.take(table, me, t)
        kind = jnp.int32(-1)
        for c, device in enumerate((me, me - info.rows, me + info.rows, me - 1, me + 1)):
            kind = jnp.where((slot >= 0) & info.local(slot, device)[0], c, kind)
        patches[t] = kind
    plan_sides(info, me, table, plan)
    zero = jnp.zeros(LAYER, F32)

    def full(value):
        return jnp.full(LAYER, value, F32)

    flat, slope = [], []
    for s in range(SPECIES):
        m, g = full(mob[s]), full(gain[s])
        flat.append(m / (1.0 + g))
        slope.append(m * g / (1.0 + g))
    rate = [full(rates[i]) for i in range(5)]

    for t in range(WORKING):

        def prepare(load, t=t):
            def layer(x, carry):
                a, i, v, p, q = (load(s, x) for s in range(SPECIES))
                half = 0.5 * (a + p + q)
                electrons = half + jnp.sqrt(half * half + 1.0)
                pi = rate[0] * a * i - rate[1] * p
                pv = rate[2] * a * v - rate[3] * q
                re = rate[4] * (i * v - 1.0)
                source = (a - pi - pv, i - pi - re, v - pv - re, p + pi, q + pv)
                at = pl.multiple_of(x * PAD, 8)
                for s, value in enumerate((a, i, v, p, q)):
                    spread = flat[s] + slope[s] * electrons
                    inverse = 1.0 / (1.0 + 6.0 * spread)
                    grid[t, s, pl.ds(at, TILES), :] = zero
                    grid[t, s, pl.ds(at + TILES, TILES), :] = value
                    fixed[t, s, x] = source[s] * inverse
                    factor[t, s, x] = spread * inverse
                return carry

            lax.fori_loop(0, B, layer, 0, unroll=4)
            for s in range(SPECIES):
                grid[t, s, pl.ds(B * PAD, TILES), :] = zero

        kind = patches[t]
        pl.when(kind == 0)(
            functools.partial(prepare, lambda s, x, t=t: own[t, s, x])
        )
        for c, src in ((1, p_xm), (2, p_xp), (3, p_ym), (4, p_yp)):
            pl.when(kind == c)(functools.partial(prepare, lambda s, x, src=src: src[s, x]))

    for copy in copies:
        copy.wait()


def stencil():
    source = lax.broadcasted_iota(jnp.int32, (256, 128), 0)
    target = lax.broadcasted_iota(jnp.int32, (256, 128), 1)
    inside = source < 128
    step = jnp.abs(source - target)
    along_z = (step == 1) & (source // B == target // B)
    across = jnp.abs(source - 128 - target) == 128 - B
    hit = (inside & (along_z | (step == B))) | (jnp.logical_not(inside) & across)
    return jnp.where(hit, 1.0, 0.0).astype(jnp.bfloat16)


def sweep_kernel(
    patches, plan, grid, fixed, factor, f_own, f_xm, f_xp, g_ym, g_yp, g_xm, g_xp, g_y2m, g_y2p,
    blank, out_ref, ghost, mid_0, mid_1, base_0, base_1, weights, stage, sems,
):
    del blank
    mids, bases = (mid_0, mid_1), (base_0, base_1)
    sub, lane = iotas()
    z = lane & (B - 1)
    z_low, z_high = z == 0, z == B - 1
    y_low = (sub == 0) & (lane < B)
    y_high = (sub == TILES - 1) & (lane >= 128 - B)
    zero = jnp.zeros(LAYER, F32)
    stage_rows = raw_rows(stage)
    weights[...] = stencil()

    def clear_pad(i, carry):
        for mid in mids:
            for a in range(2):
                mid[a, pl.ds(pl.multiple_of(i * PAD, 8), TILES), :] = zero
        return carry

    lax.fori_loop(0, B + 1, clear_pad, 0, unroll=3)

    def copy_out(s):
        return pltpu.make_async_copy(
            stage.at[s, :, pl.ds(0, WORKING), :],
            out_ref.at[s, :, pl.ds(0, WORKING), :],
            sems.at[s],
        )

    for t in range(WORKING):

        @each_side
        def _(f, t=t):
            kind = plan[t * SIDES + f]
            place = plan[WORKING * SIDES + t * SIDES + f]
            for c, src in enumerate(
                (f_own, g_ym, g_yp, g_xm, g_xp, g_y2m, g_y2p, f_xm, f_xp)
            ):
                pl.when(kind == c)(functools.partial(copy_face, ghost, t * SIDES + f, src, place))

    def add_ghosts(t, s):
        at_side = t * SIDES
        y_first, y_last = ghost[at_side + 2, s], ghost[at_side + 3, s]
        z_first, z_last = ghost[at_side + 4, s], ghost[at_side + 5, s]
        firsts = [pltpu.roll(y_first, (128 - j * B) % 128, 1) if j else y_first for j in range(4)]
        lasts = [pltpu.roll(y_last, (3 - j) * B, 1) if j < 3 else y_last for j in range(4)]
        for x in range(B):
            zf = pltpu.roll(z_first, 128 - x, 1) if x else z_first
            zl = pltpu.roll(z_last, B - 1 - x, 1) if x < B - 1 else z_last
            i, j = x // 4, x % 4
            yf = pltpu.roll(firsts[j], TILES - i, 0) if i else firsts[j]
            yl = pltpu.roll(lasts[j], TILES - 1 - i, 0) if i < TILES - 1 else lasts[j]
            outer = jnp.where(z_low, zf, jnp.where(z_high, zl, zero))
            outer = outer + jnp.where(y_low, yf, jnp.where(y_high, yl, zero))
            if x == 0:
                outer = outer + ghost[at_side, s]
            if x == B - 1:
                outer = outer + ghost[at_side + 1, s]
            bases[t][x] = fixed[t, s, x] + factor[t, s, x] * outer

    def loader(t, s, sweep):
        def load(row):
            if sweep == 0:
                return grid[t, s, pl.ds(row, TILES), :]
            return mids[t][(sweep - 1) % 2, pl.ds(row, TILES), :]

        return load

    def by_matmul(load):
        layers = []
        for x in range(B):
            at = x * PAD + TILES
            other = jnp.where(lane >= 64, load(at - 1), load(at + 1))
            layers.append(jnp.concatenate([load(at), other], axis=1))
        whole = jnp.concatenate(layers, axis=0)
        high = whole.astype(jnp.bfloat16)
        low = (whole - high.astype(F32)).astype(jnp.bfloat16)
        w = weights[...]
        sums = jnp.dot(high, w, preferred_element_type=F32)
        sums = sums + jnp.dot(low, w, preferred_element_type=F32)
        return [sums[x * TILES : (x + 1) * TILES] for x in range(B)]

    def by_rolls(load, x, here):
        at = x * PAD + TILES
        total = pltpu.roll(jnp.where(lane >= 128 - B, load(at - 1), here), B, 1)
        total = total + pltpu.roll(jnp.where(lane < B, load(at + 1), here), 128 - B, 1)
        total = total + jnp.where(z_low, zero, pltpu.roll(here, 1, 1))
        return total + jnp.where(z_high, zero, pltpu.roll(here, 127, 1))

    def one_sweep(t, s, sweep, sums, live):
        load = loader(t, s, sweep)
        before, here = None, load(TILES)
        for x in range(B):
            at = x * PAD + TILES
            after = load(at + PAD) if x < B - 1 else None
            total = by_rolls(load, x, here) if sums is None else sums[x]
            if before is not None:
                total = total + before
            if after is not None:
                total = total + after
            new = bases[t][x] + factor[t, s, x] * total
            if sweep < SWEEPS - 1:
                mids[t][sweep % 2, pl.ds(at, TILES), :] = new
            else:
                row = s * PER_S + x * PER_X + t
                stage_rows[pl.ds(row, TILES, stride=8), :] = jnp.where(live, new, zero)
            before, here = here, after

    lives = [jnp.full(LAYER, patches[t], jnp.int32) >= 0 for t in range(WORKING)]

    def species(s, carry):
        for t in range(WORKING):
            add_ghosts(t, s)
        for sweep in range(SWEEPS):
            for t in range(WORKING):
                sums = by_matmul(loader(t, s, sweep)) if t % 2 or sweep == 0 else None
                one_sweep(t, s, sweep, sums, lives[t])
        copy_out(s).start()
        return carry

    lax.fori_loop(0, SPECIES, species, 0)
    for s in range(SPECIES):
        copy_out(s).wait()


def passed_along(x, axis, by):
    devices = lax.axis_size(axis)
    pairs = [(i, i + by) for i in range(devices) if 0 <= i + by < devices]
    return lax.ppermute(x, axis, pairs)


def both_ways(up, down, axis, by):
    return passed_along(up, axis, by), passed_along(down, axis, -by)


def call(kernel, out_shape, in_specs, out_specs, scratch=(), aliases=None, mib=2):
    def run(*args):
        return pl.pallas_call(
            kernel,
            out_shape=out_shape,
            in_specs=in_specs,
            out_specs=out_specs,
            scratch_shapes=list(scratch),
            input_output_aliases=aliases or {},
            compiler_params=pltpu.CompilerParams(vmem_limit_bytes=mib << 20),
        )(*args)

    return run


def shape(*dims, dtype=F32):
    return jax.ShapeDtypeStruct(dims, dtype)


def body(concentration, neighbours, source_slot, mobility, fermi_gain, rates):
    cap, species, cells = concentration.shape
    tiles = cells // 128
    rows, columns = lax.axis_size("gy"), lax.axis_size("gx")
    me = (lax.axis_index("gx") * rows + lax.axis_index("gy")).astype(jnp.int32)[None]
    info = Table(cap, rows, rows * columns)
    view = concentration.reshape(cap, species, tiles, 128).transpose(1, 2, 0, 3)
    table = info.gather(neighbours, source_slot)

    patch = shape(species, B, *LAYER)
    two_patches = shape(WORKING, species, B, *LAYER)
    all_sides = shape(WORKING * SIDES, species, *LAYER)
    one_patch = shape(SIDES, species, *LAYER)
    dense, faces = call(
        functools.partial(pack_kernel, cap),
        (shape(SPARE * cap, species, B, *LAYER), shape(cap * SIDES, species, *LAYER)),
        [HBM],
        (HBM, VMEM),
        [
            pltpu.VMEM((species, tiles, 8, 128), F32),
            pltpu.VMEM((cap, species, B, *LAYER), F32),
            pltpu.SemaphoreType.DMA((species,)),
            pltpu.SemaphoreType.DMA((species,)),
        ],
        mib=57,
    )(view)
    s_yp, s_ym = call(
        functools.partial(first_kernel, info), (patch,) * 2, [SMEM, SMEM, HBM], (VMEM,) * 2,
        [pltpu.SemaphoreType.DMA((2,))],
        mib=50,
    )(me, table, dense)
    p_ym, p_yp = both_ways(s_yp, s_ym, "gy", 1)
    f_xm, f_xp = both_ways(faces, faces, "gx", 1)

    s_xp, s_xm, t_x2p, t_x2m, t_y2p, t_y2m, own = call(
        functools.partial(second_kernel, info),
        (patch, patch) + (one_patch,) * 4 + (two_patches,),
        [SMEM, SMEM, HBM, VMEM],
        (VMEM,) * 7,
        [pltpu.SemaphoreType.DMA((2 + WORKING,))],
        mib=50,
    )(me, table, dense, faces)
    p_xm, p_xp = both_ways(s_xp, s_xm, "gx", 1)

    t_yp, t_ym = call(
        functools.partial(faces_kernel, info),
        (all_sides,) * 2,
        [SMEM] * 2 + [VMEM] * 3,
        (VMEM,) * 2,
    )(me, table, faces, f_xm, f_xp)
    g_ym, g_yp = both_ways(t_yp, t_ym, "gy", 1)
    g_y2m, g_y2p = both_ways(t_y2p, t_y2m, "gy", 2)
    g_x2m, g_x2p = both_ways(t_x2p, t_x2m, "gx", 2)

    padded = shape(WORKING, species, B * PAD + TILES, 128)
    grid, fixed, factor, patches, plan, blank = call(
        functools.partial(prepare_kernel, info),
        (
            padded,
            two_patches,
            two_patches,
            shape(WORKING, dtype=jnp.int32),
            shape(2 * WORKING * SIDES, dtype=jnp.int32),
            shape(species, tiles, cap, 128),
        ),
        [SMEM] * 5 + [VMEM] * 5,
        (VMEM,) * 3 + (SMEM, SMEM, ANY),
        [pltpu.VMEM((tiles, 8, 128), F32), pltpu.SemaphoreType.DMA((species,))],
        mib=4,
    )(me, table, mobility, fermi_gain, rates, own, p_xm, p_xp, p_ym, p_yp)

    moved = call(
        sweep_kernel,
        shape(species, tiles, cap, 128),
        [SMEM] * 2 + [VMEM] * 12 + [ANY],
        ANY,
        [
            pltpu.VMEM((WORKING * SIDES, species, *LAYER), F32),
            pltpu.VMEM((2, B * PAD + TILES, 128), F32),
            pltpu.VMEM((2, B * PAD + TILES, 128), F32),
            pltpu.VMEM((B, *LAYER), F32),
            pltpu.VMEM((B, *LAYER), F32),
            pltpu.VMEM((256, 128), jnp.bfloat16),
            pltpu.VMEM((species, tiles, 8, 128), F32),
            pltpu.SemaphoreType.DMA((species,)),
        ],
        {14: 0},
        mib=10,
    )(
        patches, plan, grid, fixed, factor, faces, f_xm, f_xp,
        g_ym, g_yp, g_x2m, g_x2p, g_y2m, g_y2p, blank,
    )
    return moved.transpose(2, 0, 1, 3).reshape(cap, species, cells)


def solution(mesh):
    placed = (P(("gx", "gy"), None, None), P(("gx", "gy"), None), P(("gx", "gy")), P(), P(), P())
    return jax.shard_map(
        body, mesh=mesh, in_specs=placed, out_specs=P(("gx", "gy"), None, None), check_vma=False
    )
```

```python
import functools

import jax
import jax.numpy as jnp
from jax import lax
from jax.experimental import pallas as pl
from jax.experimental.pallas import tpu as pltpu
from jax.sharding import PartitionSpec as P


B = 32
SPECIES = 5
SWEEPS = 3
KEEP = 2
MOVE = 1
WORKING = KEEP - 1 + MOVE
SIDES = 6
SPARE = 4
TILES = B * B // 128
LAYER = (TILES, 128)
PAD = 2 * TILES


VMEM = pl.BlockSpec(memory_space=pltpu.VMEM)
SMEM = pl.BlockSpec(memory_space=pltpu.SMEM)
ANY = pl.BlockSpec(memory_space=pl.ANY)
HBM = pl.BlockSpec(memory_space=pltpu.HBM)
F32 = jnp.float32


def iotas():
    sub = lax.broadcasted_iota(jnp.int32, LAYER, 0)
    lane = lax.broadcasted_iota(jnp.int32, LAYER, 1)
    return sub, lane


def raw_copy(c_ref, raw, sems, cap, s):
    return pltpu.make_async_copy(c_ref.at[s], raw.at[s, :, pl.ds(0, cap), :], sems.at[s])


def raw_rows(raw):
    return raw.reshape(SPECIES * B * TILES * 8, 128)


PER_X = TILES * 8
PER_S = B * PER_X


class Table:
    def __init__(self, cap, rows, devices):
        self.cap, self.rows, self.devices = cap, rows, devices
        self.width = -(-(1 + SIDES) * cap // 8) * 8
        self.scale = -(-(1 << 16) // cap)
        assert all((p * self.scale) >> 16 == p // cap for p in range(cap * devices))

    def gather(self, neighbours, source_slot):
        sent = call(
            functools.partial(table_kernel, self),
            shape(self.devices, 1, self.width, dtype=jnp.int32),
            [SMEM, SMEM],
            VMEM,
            mib=63,
        )(source_slot, neighbours)
        return lax.all_to_all(sent, ("gx", "gy"), 0, 0, tiled=True)

    def device(self, slot):
        return (slot * self.scale) >> 16

    def there(self, device):
        return jnp.clip(device, 0, self.devices - 1)

    def take(self, table, device, t):
        return table[self.there(device), 0, t]

    def local(self, slot, device):
        at = slot - device * self.cap
        return (at >= 0) & (at < self.cap), jnp.clip(at, 0, self.cap - 1)

    def need(self, table, slot, side):
        safe = jnp.maximum(slot, 0)
        home = self.device(safe)
        near = table[home, 0, self.cap + (safe - home * self.cap) * SIDES + side]
        face = jnp.where(near < 0, side, side ^ 1)
        return jnp.where(slot < 0, -1, jnp.where(near < 0, slot, near)), face


def table_kernel(info, source_slot, neighbours, out):
    lane = lax.broadcasted_iota(jnp.int32, (1, info.width), 1)
    row = jnp.zeros((1, info.width), jnp.int32)
    for p in range(info.cap):
        row = jnp.where(lane == p, source_slot[p], row)
        for f in range(SIDES):
            row = jnp.where(lane == info.cap + p * SIDES + f, neighbours[p, f], row)
    for device in range(info.devices):
        out[device] = row


def each_side(body):
    def step(f, carry):
        body(f)
        return carry

    lax.fori_loop(0, SIDES, step, 0)


def copy_face(dst, dst_at, src, src_at):
    for s in range(SPECIES):
        dst[dst_at, s] = src[src_at, s]


def picked(info, table, me, device):
    pick = jnp.int32(0)
    for t in range(WORKING):
        here, at = info.local(info.take(table, device, t), me)
        pick = jnp.where(here, at, pick)
    return pick


def pack_kernel(cap, c_ref, dense_ref, faces, raw, dense, sems, out_sems):
    for s in range(SPECIES):
        raw_copy(c_ref, raw, sems, cap, s).start()
    rows = raw_rows(raw)
    _, lane = iotas()
    z = lane & (B - 1)
    quarter = lane // B

    def copy_out(s):
        return pltpu.make_async_copy(
            dense.at[:, s], dense_ref.at[pl.ds(0, cap), s], out_sems.at[s]
        )

    def species(s, carry):
        raw_copy(c_ref, raw, sems, cap, s).wait()
        base = s * PER_S

        for p in range(cap):
            for x in range(B):
                dense[p, s, x] = rows[pl.ds(base + x * PER_X + p, TILES, stride=8), :]
        copy_out(s).start()
        for p in range(cap):
            start = base + p
            z_first = z_last = None
            for x in range(B):
                v = dense[p, s, x]
                a = v if x == 0 else pltpu.roll(v, x, 1)
                b = v if x == B - 1 else pltpu.roll(v, 128 + x - (B - 1), 1)
                z_first = a if x == 0 else jnp.where(z == x, a, z_first)
                z_last = b if x == 0 else jnp.where(z == x, b, z_last)
                if x == 0:
                    faces[p * SIDES + 0, s] = v
                if x == B - 1:
                    faces[p * SIDES + 1, s] = v
            y_first = y_last = None
            for j in range(4):
                a = rows[pl.ds(start + j * PER_X, TILES, stride=4 * PER_X), :]
                b = rows[pl.ds(start + j * PER_X + (TILES - 1) * 8, TILES, stride=4 * PER_X), :]
                a = a if j == 0 else pltpu.roll(a, j * B, 1)
                b = b if j == 3 else pltpu.roll(b, (j + 1) * B, 1)
                y_first = a if j == 0 else jnp.where(quarter == j, a, y_first)
                y_last = b if j == 0 else jnp.where(quarter == j, b, y_last)
            faces[p * SIDES + 2, s] = y_first
            faces[p * SIDES + 3, s] = y_last
            faces[p * SIDES + 4, s] = z_first
            faces[p * SIDES + 5, s] = z_last
        return carry

    lax.fori_loop(0, SPECIES, species, 0)
    for s in range(SPECIES):
        copy_out(s).wait()


def patch_copies(pairs, dense, sems):
    return [
        pltpu.make_async_copy(dense.at[number], out, sems.at[i])
        for i, (number, out) in enumerate(pairs)
    ]


def first_kernel(info, me_ref, table, dense, to_yp, to_ym, sems):
    me = me_ref[0]
    up, down = picked(info, table, me, me + 1), picked(info, table, me, me - 1)
    copies = patch_copies(((up, to_yp), (down, to_ym)), dense, sems)
    for copy in copies:
        copy.start()
    for copy in copies:
        copy.wait()


def plan_sides(info, me, table, plan):
    my_column = me // info.rows
    my_row = me - my_column * info.rows
    for t in range(WORKING):
        slot = info.take(table, me, t)

        @each_side
        def _(f, t=t, slot=slot):
            near, face = info.need(table, slot, f)
            at = t * SIDES + f
            safe = jnp.maximum(near, 0)
            home = info.device(safe)
            column = home // info.rows
            row = home - column * info.rows
            beside = jnp.abs(column - my_column) < 2
            here = (safe - home * info.cap) * SIDES + face
            kind, place = jnp.int32(0), here
            for c, far in ((7, -info.rows), (8, info.rows)):
                kind = jnp.where(home == me + far, c, kind)
            for c, far in ((1, -1), (2, 1)):
                hit = beside & (row == my_row + far)
                kind, place = jnp.where(hit, c, kind), jnp.where(hit, at, place)
            for c, far in ((3, -2 * info.rows), (4, 2 * info.rows)):
                hit = home == me + far
                kind, place = jnp.where(hit, c, kind), jnp.where(hit, f, place)
            for c, far in ((5, -2), (6, 2)):
                hit = (column == my_column) & (row == my_row + far)
                kind, place = jnp.where(hit, c, kind), jnp.where(hit, f, place)
            plan[at] = jnp.where(near >= 0, kind, 0)
            plan[WORKING * SIDES + at] = jnp.where(near >= 0, place, 0)


def second_kernel(info, me_ref, table, dense, faces, *refs):
    to_xp, to_xm, to_x2p, to_x2m, to_y2p, to_y2m, own, sems = refs
    me = me_ref[0]
    up, down = picked(info, table, me, me + info.rows), picked(info, table, me, me - info.rows)
    kept = [info.local(info.take(table, me, t), me)[1] for t in range(WORKING)]
    pairs = [(up, to_xp), (down, to_xm), *((kept[t], own.at[t]) for t in range(WORKING))]
    copies = patch_copies(pairs, dense, sems)
    for copy in copies:
        copy.start()

    for step, out in ((info.rows, to_x2p), (-info.rows, to_x2m), (1, to_y2p), (-1, to_y2m)):
        for t in range(WORKING):
            slot = info.take(table, me + 2 * step, t)
            between, _ = info.local(slot, me + step)

            @pl.when(between)
            def _(slot=slot, out=out):
                @each_side
                def _(f):
                    near, face = info.need(table, slot, f)
                    here, at = info.local(near, me)
                    pl.when(here)(
                        functools.partial(copy_face, out, f, faces, at * SIDES + face)
                    )

    for copy in copies:
        copy.wait()


def copy_row(info, me, near, face, out, at, f_own, f_xm, f_xp):
    for shift, src in ((0, f_own), (-info.rows, f_xm), (info.rows, f_xp)):
        here, number = info.local(near, me + shift)
        pl.when((near >= 0) & here)(
            functools.partial(copy_face, out, at, src, number * SIDES + face)
        )


def faces_kernel(info, me_ref, table, f_own, f_xm, f_xp, to_yp, to_ym):
    me = me_ref[0]
    for step, out in ((1, to_yp), (-1, to_ym)):
        for t in range(WORKING):
            slot = info.take(table, me + step, t)

            @each_side
            def _(f, t=t, out=out, slot=slot):
                near, face = info.need(table, slot, f)
                copy_row(info, me, near, face, out, t * SIDES + f, f_own, f_xm, f_xp)


def prepare_kernel(
    info, me_ref, table, mob, gain, rates, own, p_xm, p_xp, p_ym, p_yp,
    grid, fixed, factor, patches, plan, blank, zeros, sems,
):
    zeros[...] = jnp.zeros(zeros.shape, F32)
    copies = [
        pltpu.make_async_copy(zeros.at[:, pl.ds(0, info.cap), :], blank.at[s], sems.at[s])
        for s in range(SPECIES)
    ]
    for copy in copies:
        copy.start()
    me = me_ref[0]
    for t in range(WORKING):
        slot = info.take(table, me, t)
        kind = jnp.int32(-1)
        for c, device in enumerate((me, me - info.rows, me + info.rows, me - 1, me + 1)):
            kind = jnp.where((slot >= 0) & info.local(slot, device)[0], c, kind)
        patches[t] = kind
    plan_sides(info, me, table, plan)
    zero = jnp.zeros(LAYER, F32)

    def full(value):
        return jnp.full(LAYER, value, F32)

    flat, slope = [], []
    for s in range(SPECIES):
        m, g = full(mob[s]), full(gain[s])
        flat.append(m / (1.0 + g))
        slope.append(m * g / (1.0 + g))
    rate = [full(rates[i]) for i in range(5)]

    for t in range(WORKING):

        def prepare(load, t=t):
            def layer(x, carry):
                a, i, v, p, q = (load(s, x) for s in range(SPECIES))
                half = 0.5 * (a + p + q)
                electrons = half + jnp.sqrt(half * half + 1.0)
                pi = rate[0] * a * i - rate[1] * p
                pv = rate[2] * a * v - rate[3] * q
                re = rate[4] * (i * v - 1.0)
                source = (a - pi - pv, i - pi - re, v - pv - re, p + pi, q + pv)
                at = pl.multiple_of(x * PAD, 8)
                for s, value in enumerate((a, i, v, p, q)):
                    spread = flat[s] + slope[s] * electrons
                    inverse = 1.0 / (1.0 + 6.0 * spread)
                    grid[t, s, pl.ds(at, TILES), :] = zero
                    grid[t, s, pl.ds(at + TILES, TILES), :] = value
                    fixed[t, s, x] = source[s] * inverse
                    factor[t, s, x] = spread * inverse
                return carry

            lax.fori_loop(0, B, layer, 0, unroll=4)
            for s in range(SPECIES):
                grid[t, s, pl.ds(B * PAD, TILES), :] = zero

        kind = patches[t]
        pl.when(kind == 0)(
            functools.partial(prepare, lambda s, x, t=t: own[t, s, x])
        )
        for c, src in ((1, p_xm), (2, p_xp), (3, p_ym), (4, p_yp)):
            pl.when(kind == c)(functools.partial(prepare, lambda s, x, src=src: src[s, x]))

    for copy in copies:
        copy.wait()


def stencil():
    source = lax.broadcasted_iota(jnp.int32, (256, 128), 0)
    target = lax.broadcasted_iota(jnp.int32, (256, 128), 1)
    inside = source < 128
    step = jnp.abs(source - target)
    along_z = (step == 1) & (source // B == target // B)
    across = jnp.abs(source - 128 - target) == 128 - B
    hit = (inside & (along_z | (step == B))) | (jnp.logical_not(inside) & across)
    return jnp.where(hit, 1.0, 0.0).astype(jnp.bfloat16)


def sweep_kernel(
    patches, plan, grid, fixed, factor, f_own, f_xm, f_xp, g_ym, g_yp, g_xm, g_xp, g_y2m, g_y2p,
    blank, out_ref, ghost, mid_0, mid_1, base_0, base_1, weights, stage, sems,
):
    del blank
    mids, bases = (mid_0, mid_1), (base_0, base_1)
    sub, lane = iotas()
    z = lane & (B - 1)
    z_low, z_high = z == 0, z == B - 1
    y_low = (sub == 0) & (lane < B)
    y_high = (sub == TILES - 1) & (lane >= 128 - B)
    zero = jnp.zeros(LAYER, F32)
    stage_rows = raw_rows(stage)
    weights[...] = stencil()

    def clear_pad(i, carry):
        for mid in mids:
            for a in range(2):
                mid[a, pl.ds(pl.multiple_of(i * PAD, 8), TILES), :] = zero
        return carry

    lax.fori_loop(0, B + 1, clear_pad, 0, unroll=3)

    def copy_out(s):
        return pltpu.make_async_copy(
            stage.at[s, :, pl.ds(0, WORKING), :],
            out_ref.at[s, :, pl.ds(0, WORKING), :],
            sems.at[s],
        )

    for t in range(WORKING):

        @each_side
        def _(f, t=t):
            kind = plan[t * SIDES + f]
            place = plan[WORKING * SIDES + t * SIDES + f]
            for c, src in enumerate(
                (f_own, g_ym, g_yp, g_xm, g_xp, g_y2m, g_y2p, f_xm, f_xp)
            ):
                pl.when(kind == c)(functools.partial(copy_face, ghost, t * SIDES + f, src, place))

    def add_ghosts(t, s):
        at_side = t * SIDES
        y_first, y_last = ghost[at_side + 2, s], ghost[at_side + 3, s]
        z_first, z_last = ghost[at_side + 4, s], ghost[at_side + 5, s]
        firsts = [pltpu.roll(y_first, (128 - j * B) % 128, 1) if j else y_first for j in range(4)]
        lasts = [pltpu.roll(y_last, (3 - j) * B, 1) if j < 3 else y_last for j in range(4)]
        for x in range(B):
            zf = pltpu.roll(z_first, 128 - x, 1) if x else z_first
            zl = pltpu.roll(z_last, B - 1 - x, 1) if x < B - 1 else z_last
            i, j = x // 4, x % 4
            yf = pltpu.roll(firsts[j], TILES - i, 0) if i else firsts[j]
            yl = pltpu.roll(lasts[j], TILES - 1 - i, 0) if i < TILES - 1 else lasts[j]
            outer = jnp.where(z_low, zf, jnp.where(z_high, zl, zero))
            outer = outer + jnp.where(y_low, yf, jnp.where(y_high, yl, zero))
            if x == 0:
                outer = outer + ghost[at_side, s]
            if x == B - 1:
                outer = outer + ghost[at_side + 1, s]
            bases[t][x] = fixed[t, s, x] + factor[t, s, x] * outer

    def loader(t, s, sweep):
        def load(row):
            if sweep == 0:
                return grid[t, s, pl.ds(row, TILES), :]
            return mids[t][(sweep - 1) % 2, pl.ds(row, TILES), :]

        return load

    def by_matmul(load):
        layers = []
        for x in range(B):
            at = x * PAD + TILES
            other = jnp.where(lane >= 64, load(at - 1), load(at + 1))
            layers.append(jnp.concatenate([load(at), other], axis=1))
        whole = jnp.concatenate(layers, axis=0)
        high = whole.astype(jnp.bfloat16)
        low = (whole - high.astype(F32)).astype(jnp.bfloat16)
        w = weights[...]
        sums = jnp.dot(high, w, preferred_element_type=F32)
        sums = sums + jnp.dot(low, w, preferred_element_type=F32)
        return [sums[x * TILES : (x + 1) * TILES] for x in range(B)]

    def by_rolls(load, x, here):
        at = x * PAD + TILES
        total = pltpu.roll(jnp.where(lane >= 128 - B, load(at - 1), here), B, 1)
        total = total + pltpu.roll(jnp.where(lane < B, load(at + 1), here), 128 - B, 1)
        total = total + jnp.where(z_low, zero, pltpu.roll(here, 1, 1))
        return total + jnp.where(z_high, zero, pltpu.roll(here, 127, 1))

    def one_sweep(t, s, sweep, sums, live):
        load = loader(t, s, sweep)
        before, here = None, load(TILES)
        for x in range(B):
            at = x * PAD + TILES
            after = load(at + PAD) if x < B - 1 else None
            total = by_rolls(load, x, here) if sums is None else sums[x]
            if before is not None:
                total = total + before
            if after is not None:
                total = total + after
            new = bases[t][x] + factor[t, s, x] * total
            if sweep < SWEEPS - 1:
                mids[t][sweep % 2, pl.ds(at, TILES), :] = new
            else:
                row = s * PER_S + x * PER_X + t
                stage_rows[pl.ds(row, TILES, stride=8), :] = jnp.where(live, new, zero)
            before, here = here, after

    lives = [jnp.full(LAYER, patches[t], jnp.int32) >= 0 for t in range(WORKING)]

    def species(s, carry):
        for t in range(WORKING):
            add_ghosts(t, s)
        for sweep in range(SWEEPS):
            for t in range(WORKING):
                sums = by_matmul(loader(t, s, sweep)) if t % 2 or sweep == 0 else None
                one_sweep(t, s, sweep, sums, lives[t])
        copy_out(s).start()
        return carry

    lax.fori_loop(0, SPECIES, species, 0)
    for s in range(SPECIES):
        copy_out(s).wait()


def passed_along(x, axis, by):
    devices = lax.axis_size(axis)
    pairs = [(i, i + by) for i in range(devices) if 0 <= i + by < devices]
    return lax.ppermute(x, axis, pairs)


def both_ways(up, down, axis, by):
    return passed_along(up, axis, by), passed_along(down, axis, -by)


def call(kernel, out_shape, in_specs, out_specs, scratch=(), aliases=None, mib=2):
    def run(*args):
        return pl.pallas_call(
            kernel,
            out_shape=out_shape,
            in_specs=in_specs,
            out_specs=out_specs,
            scratch_shapes=list(scratch),
            input_output_aliases=aliases or {},
            compiler_params=pltpu.CompilerParams(vmem_limit_bytes=mib << 20),
        )(*args)

    return run


def shape(*dims, dtype=F32):
    return jax.ShapeDtypeStruct(dims, dtype)


def body(concentration, neighbours, source_slot, mobility, fermi_gain, rates):
    cap, species, cells = concentration.shape
    tiles = cells // 128
    rows, columns = lax.axis_size("gy"), lax.axis_size("gx")
    me = (lax.axis_index("gx") * rows + lax.axis_index("gy")).astype(jnp.int32)[None]
    info = Table(cap, rows, rows * columns)
    view = concentration.reshape(cap, species, tiles, 128).transpose(1, 2, 0, 3)
    table = info.gather(neighbours, source_slot)

    patch = shape(species, B, *LAYER)
    two_patches = shape(WORKING, species, B, *LAYER)
    all_sides = shape(WORKING * SIDES, species, *LAYER)
    one_patch = shape(SIDES, species, *LAYER)
    dense, faces = call(
        functools.partial(pack_kernel, cap),
        (shape(SPARE * cap, species, B, *LAYER), shape(cap * SIDES, species, *LAYER)),
        [HBM],
        (HBM, VMEM),
        [
            pltpu.VMEM((species, tiles, 8, 128), F32),
            pltpu.VMEM((cap, species, B, *LAYER), F32),
            pltpu.SemaphoreType.DMA((species,)),
            pltpu.SemaphoreType.DMA((species,)),
        ],
        mib=57,
    )(view)
    s_yp, s_ym = call(
        functools.partial(first_kernel, info), (patch,) * 2, [SMEM, SMEM, HBM], (VMEM,) * 2,
        [pltpu.SemaphoreType.DMA((2,))],
        mib=50,
    )(me, table, dense)
    p_ym, p_yp = both_ways(s_yp, s_ym, "gy", 1)
    f_xm, f_xp = both_ways(faces, faces, "gx", 1)

    s_xp, s_xm, t_x2p, t_x2m, t_y2p, t_y2m, own = call(
        functools.partial(second_kernel, info),
        (patch, patch) + (one_patch,) * 4 + (two_patches,),
        [SMEM, SMEM, HBM, VMEM],
        (VMEM,) * 7,
        [pltpu.SemaphoreType.DMA((2 + WORKING,))],
        mib=50,
    )(me, table, dense, faces)
    p_xm, p_xp = both_ways(s_xp, s_xm, "gx", 1)

    t_yp, t_ym = call(
        functools.partial(faces_kernel, info),
        (all_sides,) * 2,
        [SMEM] * 2 + [VMEM] * 3,
        (VMEM,) * 2,
    )(me, table, faces, f_xm, f_xp)
    g_ym, g_yp = both_ways(t_yp, t_ym, "gy", 1)
    g_y2m, g_y2p = both_ways(t_y2p, t_y2m, "gy", 2)
    g_x2m, g_x2p = both_ways(t_x2p, t_x2m, "gx", 2)

    padded = shape(WORKING, species, B * PAD + TILES, 128)
    grid, fixed, factor, patches, plan, blank = call(
        functools.partial(prepare_kernel, info),
        (
            padded,
            two_patches,
            two_patches,
            shape(WORKING, dtype=jnp.int32),
            shape(2 * WORKING * SIDES, dtype=jnp.int32),
            shape(species, tiles, cap, 128),
        ),
        [SMEM] * 5 + [VMEM] * 5,
        (VMEM,) * 3 + (SMEM, SMEM, ANY),
        [pltpu.VMEM((tiles, 8, 128), F32), pltpu.SemaphoreType.DMA((species,))],
        mib=4,
    )(me, table, mobility, fermi_gain, rates, own, p_xm, p_xp, p_ym, p_yp)

    moved = call(
        sweep_kernel,
        shape(species, tiles, cap, 128),
        [SMEM] * 2 + [VMEM] * 12 + [ANY],
        ANY,
        [
            pltpu.VMEM((WORKING * SIDES, species, *LAYER), F32),
            pltpu.VMEM((2, B * PAD + TILES, 128), F32),
            pltpu.VMEM((2, B * PAD + TILES, 128), F32),
            pltpu.VMEM((B, *LAYER), F32),
            pltpu.VMEM((B, *LAYER), F32),
            pltpu.VMEM((256, 128), jnp.bfloat16),
            pltpu.VMEM((species, tiles, 8, 128), F32),
            pltpu.SemaphoreType.DMA((species,)),
        ],
        {14: 0},
        mib=10,
    )(
        patches, plan, grid, fixed, factor, faces, f_xm, f_xp,
        g_ym, g_yp, g_x2m, g_x2p, g_y2m, g_y2p, blank,
    )
    return moved.transpose(2, 0, 1, 3).reshape(cap, species, cells)


def solution(mesh):
    placed = (P(("gx", "gy"), None, None), P(("gx", "gy"), None), P(("gx", "gy")), P(), P(), P())
    return jax.shard_map(
        body, mesh=mesh, in_specs=placed, out_specs=P(("gx", "gy"), None, None), check_vma=False
    )
```
